32 devices in a mesh: member: 2 (over x), lon: 8 (over z, y), lat: 2 (over core).
Axes of the slice: x: 2, y: 2, z: 4, core: 2. Of those that a mesh axis runs over, the one named last changes fastest.
Arguments:
- strain_rate: float32 [3, 256, 2160], P(None, 'lon', 'lat'), may hold values from -6 to 6
- stress_start: float32 [3, 256, 2160], P(None, 'lon', 'lat'), may hold values from -3 to 3
- concentration: float32 [256, 2160], P('lon', 'lat'), may hold values from 0.5 to 1
- cell_class: int32 [512, 2160], P(('member', 'lon'), 'lat'), parts along dimension 0, may hold values from 0 to 7
- land_mask: int32 [256, 2160], P('lon', 'lat'), may hold values 0 or 1
- fold_partner: int32 [256], replicated, may hold values from 0 to 255, each once
- kernel_weights: float32 [7, 7], replicated, may hold values from 0.05 to 0.5
Outputs:
- stress_out: float32 [3, 512, 2160], P(None, ('member', 'lon'), 'lat'), parts along dimension 1
- damage_out: float32 [512, 2160], P(('member', 'lon'), 'lat'), parts along dimension 0
- mean_overstress: float32 [6], P('member'), parts along dimension 0
The draws below stay inside these ranges and needn't reach their ends.
There are 2 independent parts, one for each index of `member`. The reference program is written for one: setup_inputs(seed, part) draws one part's arguments, and reference() takes and returns one part's arrays. A program takes and returns all parts, laid end to end along the dimension named above; an argument that names none is the same for every part. Nothing has to cross between parts.
Inputs may be any that keep to these rules, and one draw needn't show every extreme that they name: `fold_partner`: each of the 256 longitude indices appears once.
All inputs are finite; a program needn't handle non-finite values. No bound on the sum of `land_mask` on one device may be relied on, other than what follows from the above.
Results may differ from the reference program's by a relative error of at most 0.0001.
Values sent between devices are 32-bit elements; how exact they have to be, the bound alone decides.
A program may use at most 64 MiB of HBM per device.

```python
import math
import jax
import jax.numpy as jnp

ITERS = 3
KW = 7
NLON = 256
NLAT = 2160


def set_ends(result, key, least, top_value):
    longest = result.shape.index(max(result.shape))
    spots = []
    for shift in (0, 1):
        where = [jax.random.randint(jax.random.fold_in(key, axis), (), 0, length) for axis, length in enumerate(result.shape)]
        where[longest] = (where[longest] + shift) % result.shape[longest]
        spots.append(tuple(where))
    return result.at[spots[0]].set(least).at[spots[1]].set(top_value)


def shard_levels(own_key, extent, shards, low, top_value):
    def one(position, blocks):
        steps = jax.random.uniform(jax.random.fold_in(jax.random.fold_in(own_key, 6), position), (blocks,), jnp.float32, low / len(shards), top_value / len(shards))
        return jnp.repeat(jnp.exp(steps), extent[position] // blocks).reshape((-1,) + (1,) * (len(extent) - position - 1))

    gain = one(*shards[0])
    for cut in shards[1:]:
        gain = gain * one(*cut)
    return gain


def scatter_about(stream_key, extent, scale, most, pieces=(), dtype=jnp.bfloat16):
    gain = shard_levels(stream_key, extent, pieces, -0.22, 0.18) if pieces else 1.0
    values = jax.random.normal(stream_key, extent, jnp.float32) * scale * gain
    return jnp.minimum(jnp.maximum(values, -most), most).astype(dtype)


def setup_inputs(seed: int = 0, part: int = 0) -> dict:
    streams_of = jax.random.split(jax.random.key(seed), 8)
    part_splits = jax.random.split(jax.random.fold_in(streams_of[7], part), 8)
    return {
        "strain_rate": scatter_about(streams_of[0], (3, NLON, NLAT), 1.0, 6.0, ((1, 8), (2, 2)), jnp.float32),
        "stress_start": scatter_about(streams_of[1], (3, NLON, NLAT), 0.5, 3.0, ((1, 8), (2, 2)), jnp.float32),
        "concentration": jnp.clip(0.5 + 0.5 * jax.random.uniform(streams_of[2], (NLON, NLAT), jnp.float32) ** shard_levels(streams_of[2], (NLON, NLAT), ((0, 8), (1, 2)), -0.2, 0.2), 0.5, 1.0),
        "cell_class": set_ends(jax.random.randint(part_splits[3], (NLON, NLAT), 0, 8), jax.random.fold_in(part_splits[3], 1), 0, 7).astype(jnp.int32),
        "land_mask": set_ends((jax.random.randint(streams_of[4], (NLON, NLAT), 0, 4) < 3).astype(jnp.int32), jax.random.fold_in(streams_of[4], 1), 0, 1),
        "fold_partner": jax.random.permutation(streams_of[5], NLON).astype(jnp.int32),
        "kernel_weights": jnp.clip(jnp.exp(jax.random.uniform(streams_of[6], (KW, KW), jnp.float32, math.log(0.05), math.log(0.5))), 0.05, 0.5),
    }


def extend(fields, partner, width):
    top = fields[:, :, -width:]
    north = jnp.take(top, partner, axis=1)[:, :, ::-1]
    south = jnp.zeros_like(north)
    tall = jnp.concatenate([south, fields, north], axis=2)
    return jnp.concatenate([tall[:, -width:], tall, tall[:, :width]], axis=1)

def smooth(padded, weights, ncols, nrows):
    side = weights.shape[0]
    total = jnp.zeros((padded.shape[0], ncols, nrows), jnp.float32)
    for first in range(side):
        for second in range(side):
            total = total + weights[first, second] * padded[:, first:first + ncols, second:second + nrows]
    return total

def reference(strain_rate, stress_start, concentration, cell_class, land_mask, fold_partner, kernel_weights):
    width = kernel_weights.shape[0] // 2
    ocean = land_mask.astype(jnp.float32)
    ncols, nrows = ocean.shape
    denom = smooth(extend(ocean[None], fold_partner, width), kernel_weights, ncols, nrows)[0] + 1.0
    count = jnp.sum(ocean)
    damage = ocean * 0.1 * cell_class.astype(jnp.float32) * concentration
    stress = ocean[None] * stress_start
    base = concentration * jnp.exp(-2.0 * (1.0 - concentration))
    e_one, e_two, e_shear = (strain_rate[0], strain_rate[1], strain_rate[2])
    load = jnp.stack([e_one + e_two / 3.0, e_two + e_one / 3.0, e_shear / (4.0 / 3.0)]) / (8.0 / 9.0)
    means = []
    for step in range(ITERS):
        keep = 1.0 - damage
        theta = 0.5 / (keep * keep)
        elastic = ocean[None] * (stress + (base * keep)[None] * load) / (1.0 + theta)[None]
        half_diff = (elastic[0] - elastic[1]) / 2.0
        tau = jnp.sqrt(half_diff * half_diff + elastic[2] * elastic[2] + 0.25)
        ratio = (tau + 0.7 * (elastic[0] + elastic[1]) / 2.0) / (0.6 * concentration)
        over = jnp.maximum(ratio, 1.0)
        q_part = 1.0 - 1.0 / over
        mean_now = jnp.sum(ocean * (over - 1.0)) / (count + 1.0)
        means.append(mean_now)
        factor = 1.0 / (1.0 + 2.0 * mean_now)
        local_damage = ocean * (damage + factor * keep * q_part)
        local_stress = elastic * (1.0 - factor * q_part)[None]
        fields = jnp.concatenate([local_damage[None], local_stress], axis=0)
        averaged = smooth(extend(fields, fold_partner, width), kernel_weights, ncols, nrows) / denom[None]
        fresh = ocean[None] * (0.5 * fields + 0.5 * averaged)
        damage = fresh[0]
        stress = fresh[1:]
    return (stress, damage, jnp.stack(means).astype(jnp.float32))
```

```python
import functools

import jax
import jax.numpy as jnp
from jax import lax
from jax.experimental import pallas as pl
from jax.experimental.pallas import tpu as pltpu
from jax.sharding import PartitionSpec as P

ITERS = 3
LANES = 128
SUB = 8
NORTH = 66
MESH = pl.DeviceIdType.MESH
F32 = jnp.float32


def kernel(
    nlon, nlat, nrows, R, L, side,
    w_hbm, partner_hbm, e_hbm, s_hbm, conc_hbm, class_hbm, mask_hbm,
    stress_ref, damage_ref, mean_ref,
    w_ref, partner_ref, where_ref,
    Z, Y, X, load, base, ocean, orl, half_ocean, half_rden, state,
    rows_out, rows_in, fixed_out, fixed_in, fixed_rows, HQ, WR, WC, C, rden_rows,
    slab, lat_in, fold_in, tops, D, T, stat, stat_in, stage,
    e_ref, s_ref, conc_ref, class_ref, mask_ref,
    in_sem, fixed_send, fixed_recv, row_send, row_recv, slab_send, lat_recv, fold_recv, stat_send, stat_recv,
):
    width = side // 2
    n = nlon * nlat
    ncols = R * SUB
    tiles = L // LANES
    lon, lat = lax.axis_index("lon"), lax.axis_index("lat")
    member = lax.axis_index("member")
    is_last = lat == nlat - 1
    me = lon * nlat + lat
    nb = nrows - (L - LANES)

    def dev(a, b):
        return (member, a, b)

    def peer(d):
        other = lax.rem(me + d, n)
        return dev(other // nlat, lax.rem(other, nlat))

    def every(first, last, body):
        if last - first <= 16:
            for d in range(first, last):
                body(d)
        else:
            lax.fori_loop(first, last, lambda d, c: (body(d), c)[1], 0)

    def tile(x, t):
        return x[:, t * LANES : (t + 1) * LANES]

    right, left = lax.rem(lon + 1, nlon), lax.rem(lon + nlon - 1, nlon)
    other_lat = lax.rem(lat + 1, nlat)

    loads = [
        pltpu.make_async_copy(a, b, in_sem.at[k])
        for k, (a, b) in enumerate((
            (mask_hbm, mask_ref), (conc_hbm, conc_ref), (class_hbm, class_ref), (s_hbm, s_ref), (e_hbm, e_ref),
            (w_hbm, w_ref), (partner_hbm, partner_ref),
        ))
    ]
    for copy in loads:
        copy.start()
    barrier = pltpu.get_barrier_semaphore()
    every(1, n, lambda d: pl.semaphore_signal(barrier, inc=1, device_id=peer(d), device_id_type=MESH))

    sub = lax.broadcasted_iota(jnp.int32, (SUB, LANES), 0)
    sub_wide = lax.broadcasted_iota(jnp.int32, (SUB, L), 0)
    lane = lax.broadcasted_iota(jnp.int32, (SUB, LANES), 1)
    slot = lax.rem(lane, width)
    packed_slot = lax.rem(lax.rem(lane, 16), width)

    edge = jnp.zeros((SUB, LANES), F32)
    for r in range(R):
        for ref in (base.at[r], ocean.at[r], orl.at[r], *(load.at[k, r] for k in range(3)), Z.at[0, r],
                    *(state.at[k, r] for k in range(3))):
            ref[:, L - LANES :] = edge
    for t in range(tiles):
        for it in range(ITERS):
            rows_in[it, t, SUB * width :, :] = edge
        fixed_rows[t] = edge
    mean_ref[...] = edge
    for copy in loads[5:]:
        copy.wait()
    for d in range(width):
        for b in range(side):
            WR[d * side + b] = jnp.where(sub < 4, w_ref[d, b], w_ref[side - 1 - d, b])
    span_lanes = 5 * width
    for d in range(1, width + 1):
        keep = (slot >= width - d) & ((lane < span_lanes) | ((lane >= NORTH) & (lane < NORTH + span_lanes)))
        for a in range(side):
            WC[(d - 1) * side + a] = jnp.where(
                keep, jnp.where(lane < NORTH - width, w_ref[a, width - d], w_ref[a, width + d]), 0.0
            )
    for i in range(ncols + 2 * width):
        p = partner_ref[lax.rem(lon * ncols + i - width + nlon * ncols, nlon * ncols)]
        col = lax.rem(p, ncols)
        where_ref[i] = ((p // ncols) * R + lax.rem(col, R)) * SUB + col // R
    for copy in loads[:5]:
        copy.wait()

    span = [min(LANES, nrows - t * LANES) for t in range(tiles)]
    sources = (
        mask_ref, conc_ref, class_ref, s_ref.at[0], s_ref.at[1], s_ref.at[2], e_ref.at[0], e_ref.at[1], e_ref.at[2]
    )
    count = jnp.zeros((SUB, LANES), F32)
    for t in range(tiles):
        cut = slice(t * LANES, t * LANES + span[t])
        for k, source in enumerate(sources):
            stage[k, t, :, : span[t]] = source[:, cut].astype(F32)
        for r in range(R):
            oc, conc, grade, s1, s2, s3, one, two, shear = (
                stage[k, t, pl.ds(r, SUB, stride=R), :][:, : span[t]] for k in range(9)
            )
            ocean[r, :, cut] = oc
            base[r, :, cut] = conc * jnp.exp(-2.0 * (1.0 - conc))
            orl[r, :, cut] = oc / (0.6 * conc)
            Z[0, r, :, cut] = oc * 0.1 * grade * conc
            for k, part in enumerate((s1, s2, s3)):
                state[k, r, :, cut] = oc * part
            load[0, r, :, cut] = (one + two / 3.0) / (8.0 / 9.0)
            load[1, r, :, cut] = (two + one / 3.0) / (8.0 / 9.0)
            load[2, r, :, cut] = (shear / (4.0 / 3.0)) / (8.0 / 9.0)
    for m in range(width):
        fixed_out[0, 0, m : m + 1, :] = orl[R - width + m, SUB - 1 : SUB, :]
        fixed_out[0, 1, m : m + 1, :] = ocean[R - width + m, SUB - 1 : SUB, :]
        fixed_out[1, 0, m : m + 1, :] = orl[width - 1 - m, 0:1, :]
        fixed_out[1, 1, m : m + 1, :] = ocean[width - 1 - m, 0:1, :]
    for r in range(R):
        oc = ocean[r]
        Z[8, r] = oc
        half_ocean[r] = 0.5 * oc
        for t in range(tiles):
            count = count + tile(oc, t)
    count = jnp.sum(count, axis=0, keepdims=True)

    pl.semaphore_wait(barrier, n - 1)

    def fixed_copy(k, to):
        return pltpu.make_async_remote_copy(
            src_ref=fixed_out.at[k, :, pl.ds(0, width), :], dst_ref=fixed_in.at[k, :, pl.ds(0, width), :],
            send_sem=fixed_send, recv_sem=fixed_recv, device_id=dev(to, lat), device_id_type=MESH,
        )

    def far_first(up, down):
        odd = lax.rem(lon, 2) == 1

        @pl.when(odd)
        def _():
            up()
            down()

        @pl.when(jnp.logical_not(odd))
        def _():
            down()
            up()

    far_first(lambda: fixed_copy(0, right).start(), lambda: fixed_copy(1, left).start())

    def conv(f, c):
        for r in range(R):
            X[width + r] = Z[f, r]
        for m in range(width):
            X[m] = jnp.where(sub_wide == 0, 0.0, pltpu.roll(Z[f, m + R - width], 1, 0))
            X[R + width + m] = jnp.where(sub_wide == SUB - 1, 0.0, pltpu.roll(Z[f, m], SUB - 1, 0))
        for b in range(side):
            acc = [None] * R
            for p in range(R + 2 * width):
                x = X[p]
                for r in range(R):
                    a = p - r
                    if 0 <= a < side:
                        term = w_ref[a, b] * x
                        acc[r] = term if acc[r] is None else acc[r] + term
            for r in range(R):
                moved = acc[r] if b == width else pltpu.roll(acc[r], (width - b) % L, 1)
                if b == 0:
                    Y[f, r] = moved
                else:
                    Y[f, r] = Y[f, r] + moved
        return c

    def row_terms(halos):
        for r in range(width):
            total = None
            for b in range(side):
                parts = []
                for t in range(tiles):
                    acc = None
                    for m in range(r, width):
                        term = WR[(m - r) * side + b] * halos[m][t]
                        acc = term if acc is None else acc + term
                    parts.append(acc)
                wide = jnp.concatenate(parts, axis=1)
                wide = wide if b == width else pltpu.roll(wide, (width - b) % L, 1)
                total = wide if total is None else total + wide
            yield r, total

    def row_term(p, f, t):
        cut = slice(t * LANES, (t + 1) * LANES)
        out = jnp.zeros((SUB, LANES), F32)
        if p < width:
            out = jnp.where(sub == 0, C[p, f : f + 1, cut], out)
        if R - 1 - p < width:
            out = jnp.where(sub == SUB - 1, C[R - 1 - p, 4 + f : 5 + f, cut], out)
        return out

    def flip(x, at):
        y = jnp.where(at == 0, pltpu.roll(x, LANES - (width - 1), 1), x)
        return jnp.where(at == width - 1, pltpu.roll(x, width - 1, 1), y)

    def column_term(f, p):
        at = width * f + width
        south = jnp.where(lane < width, pltpu.roll(T[0, p], (LANES - at) % LANES, 1), 0.0)
        north = jnp.where(
            (lane >= nb - width) & (lane < nb), pltpu.roll(T[1, p], (nb - width - NORTH - at) % LANES, 1), 0.0
        )
        return south, north

    def iteration(it, carry):
        excess = jnp.zeros((SUB, LANES), F32)
        for r in range(R):
            oc = ocean[r]
            damage = Z[0, r]
            keep = 1.0 - damage
            square = keep * keep
            scale = oc * square / (square + 0.5)
            bk = base[r] * keep
            el = [scale * (state[k, r] + bk * load[k, r]) for k in range(3)]
            half = (el[0] - el[1]) * 0.5
            tau = jnp.sqrt(half * half + el[2] * el[2] + 0.25)
            over = jnp.maximum((tau + 0.35 * (el[0] + el[1])) * orl[r], 1.0)
            q = 1.0 - 1.0 / over
            for t in range(tiles):
                excess = excess + (tile(over, t) - 1.0)
            Z[4, r] = keep * q
            for k in range(3):
                Z[1 + k, r] = el[k]
                Z[5 + k, r] = -(el[k] * q)
            for m in range(width):
                for f, part in enumerate((damage, *el)):
                    for t in range(tiles):
                        if r == R - width + m:
                            rows_out[it, t, SUB * m + f : SUB * m + f + 1, :] = tile(part, t)[SUB - 1 : SUB]
                        if r == width - 1 - m:
                            rows_out[it, t, SUB * m + 4 + f : SUB * m + 5 + f, :] = tile(part, t)[0:1]
        stat[it, 0:1, :] = jnp.sum(excess, axis=0, keepdims=True)
        stat[it, 1:2, :] = count

        def stat_copy(d):
            return pltpu.make_async_remote_copy(
                src_ref=stat.at[it], dst_ref=stat_in.at[it, d], send_sem=stat_send,
                recv_sem=stat_recv.at[it], device_id=peer(d), device_id_type=MESH,
            )

        every(1, n, lambda d: stat_copy(d).start())

        low = jnp.zeros((SUB, LANES), F32)
        high = jnp.zeros((SUB, LANES), F32)
        for r in range(R):
            for f in range(9):
                at = 32 * r + (width * f if f < 4 else (16 + width * (f - 4) if f < 8 else 4 * width))
                here = (lane >= at) & (lane < at + width)
                low = jnp.where(here, pltpu.roll(Z[f, r, :, :LANES], at, 1), low)
                high = jnp.where(here, pltpu.roll(Z[f, r, :, L - LANES :], (at + width - nb) % LANES, 1), high)
        slab[it, 0] = jnp.where(is_last, low, high)
        slab[it, 1] = high

        def lat_copy(k):
            to = lax.rem(lon + 1 - k + nlon, nlon)
            return pltpu.make_async_remote_copy(
                src_ref=slab.at[it, 0], dst_ref=lat_in.at[it, k], send_sem=slab_send,
                recv_sem=lat_recv.at[it], device_id=dev(to, other_lat), device_id_type=MESH,
            )

        def fold_copy(d):
            return pltpu.make_async_remote_copy(
                src_ref=slab.at[it, 1], dst_ref=fold_in.at[it, lon],
                send_sem=slab_send, recv_sem=fold_recv.at[it],
                device_id=dev(lax.rem(lon + d, nlon), lat), device_id_type=MESH,
            )

        @pl.when(is_last)
        def _():
            every(1, nlon, lambda d: fold_copy(d).start())
            fold_in[it, lon] = slab[it, 1]

        for k in range(3):
            lat_copy(k).start()

        def row_copy(s, m, to):
            piece = pl.ds(SUB * m + 4 * s, 4)
            return pltpu.make_async_remote_copy(
                src_ref=rows_out.at[it, :, piece, :], dst_ref=rows_in.at[it, :, piece, :], send_sem=row_send,
                recv_sem=row_recv.at[it], device_id=dev(to, lat), device_id_type=MESH,
            )

        def start_rows(s, to):
            for m in range(width):
                row_copy(s, m, to).start()

        far_first(lambda: start_rows(0, right), lambda: start_rows(1, left))

        lax.fori_loop(0, jnp.where(it == 0, 9, 8), conv, 0)

        def drain(ref, sem):
            pltpu.make_async_copy(ref, ref, sem).wait()

        def wait_halos():
            drain(rows_in.at[it, :, pl.ds(0, SUB * width), :], row_recv.at[it])
            drain(lat_in.at[it], lat_recv.at[it])

            @pl.when(is_last)
            def _():
                drain(fold_in.at[it, pl.ds(0, nlon - 1)], fold_recv.at[it])

        drain(stat_in.at[it, pl.ds(1, n - 1)], stat_recv.at[it])
        total = stat[it]
        if n <= 16:
            for d in range(1, n):
                total = total + stat_in[it, d]
        else:
            total = lax.fori_loop(1, n, lambda d, c: c + stat_in[it, d], total)
        sums = jnp.sum(total, axis=1, keepdims=True)
        mean = sums[0:1] / (sums[1:2] + 1.0)
        factor = 1.0 / (1.0 + 2.0 * mean)
        mean_ref[...] = jnp.where(lane == it, mean, mean_ref[...])

        def columns():
            @pl.when(is_last)
            def _():
                def spread(k):
                    got = fold_in[it, k]
                    got = got + factor * pltpu.roll(got, LANES - 16, 1)
                    for r in range(R):
                        tops[pl.ds((k * R + r) * SUB, SUB), :] = pltpu.roll(got, (NORTH - 32 * r) % LANES, 1)

                every(0, nlon, spread)
                for i in range(ncols + 2 * width):
                    D[i : i + 1, :] = tops[pl.ds(where_ref[i], 1), :]

            south_side = lane < NORTH - width
            own = []
            for k in range(3):
                got = lat_in[it, k]
                got = got + factor * pltpu.roll(got, LANES - 16, 1)
                own.append(jnp.where(is_last, got, flip(got, packed_slot)))

            def piece(k, r):
                return jnp.where(
                    is_last, pltpu.roll(own[k], (LANES - 32 * r) % LANES, 1),
                    pltpu.roll(own[k], (NORTH - 32 * r) % LANES, 1),
                )

            mid = [piece(1, r) for r in range(R)]
            ghosts = [None] * (R + 2 * width)
            for r in range(R):
                ghosts[width + r] = mid[r]
            for m in range(width):
                r = m + R - width
                ghosts[m] = jnp.where(sub == 0, pltpu.roll(piece(0, r), 1, 0), pltpu.roll(mid[r], 1, 0))
                ghosts[R + width + m] = jnp.where(
                    sub == SUB - 1, pltpu.roll(piece(2, m), SUB - 1, 0), pltpu.roll(mid[m], SUB - 1, 0)
                )
            for p in range(R + 2 * width):
                fold = D[pl.ds(p, SUB, stride=R), :]
                ghosts[p] = jnp.where(
                    south_side, jnp.where(is_last, ghosts[p], 0.0), jnp.where(is_last, fold, ghosts[p])
                )
            for r in range(R):
                total = None
                for d in range(1, width + 1):
                    acc = None
                    for a in range(side):
                        term = WC[(d - 1) * side + a] * ghosts[r + a]
                        acc = term if acc is None else acc + term
                    acc = pltpu.roll(acc, d, 1)
                    total = acc if total is None else total + acc
                T[0, r] = total
                T[1, r] = flip(total, slot)

        def finish_ocean():
            drain(fixed_in.at[:, :, pl.ds(0, width), :], fixed_recv)
            drain(fixed_in.at[:, :, pl.ds(0, width), :], fixed_send)
            for t in range(tiles):
                cut = slice(t * LANES, (t + 1) * LANES)
                for m in range(width):
                    for s in range(2):
                        fixed_rows[t, 2 * m + s : 2 * m + s + 1, :] = fixed_in[s, 0, m : m + 1, cut]
            halos = [
                [
                    jnp.where(
                        sub < 4, fixed_in[0, 1, m : m + 1, t * LANES : (t + 1) * LANES],
                        fixed_in[1, 1, m : m + 1, t * LANES : (t + 1) * LANES],
                    )
                    for t in range(tiles)
                ]
                for m in range(width)
            ]
            for r, total in row_terms(halos):
                C[r] = total
            for r in range(R):
                south, north = column_term(4, r)
                for t in range(tiles):
                    cut = slice(t * LANES, (t + 1) * LANES)
                    denom = Y[8, r, :, cut] + row_term(r, 0, t)
                    if t == 0:
                        denom = denom + south
                    if t == tiles - 1:
                        denom = denom + north
                    half_rden[r, :, cut] = half_ocean[r, :, cut] / (denom + 1.0)
            for r in range(width):
                rden_rows[r] = jnp.where(
                    sub_wide < 4, half_rden[r, 0:1, :], half_rden[R - 1 - r, SUB - 1 : SUB, :]
                )

        @pl.when(it == 0)
        def _():
            wait_halos()
            columns()
            finish_ocean()

        for r in range(R):
            for t in range(tiles):
                cut = slice(t * LANES, (t + 1) * LANES)
                ho, hr = half_ocean[r, :, cut], half_rden[r, :, cut]
                for f in range(4):
                    local = Z[f, r, :, cut] + factor * Z[4 + f, r, :, cut]
                    spread_out = Y[f, r, :, cut] + factor * Y[4 + f, r, :, cut]
                    fresh = ho * local + hr * spread_out
                    if f == 0:
                        Z[0, r, :, cut] = fresh
                    else:
                        state[f - 1, r, :, cut] = fresh

        @pl.when(it > 0)
        def _():
            wait_halos()
            columns()

        for t in range(tiles):
            e = [rows_in[it, t, pl.ds(k, SUB, stride=4), :] for k in range(1, 4)]
            half = (e[0] - e[1]) * 0.5
            tau = jnp.sqrt(half * half + e[2] * e[2] + 0.25)
            over = jnp.maximum((tau + 0.35 * (e[0] + e[1])) * fixed_rows[t], 1.0)
            HQ[t] = factor * (1.0 - 1.0 / over)
        halos = [[None] * tiles for _ in range(width)]
        head = (sub == 0) | (sub == 4)
        for m in range(width):
            for t in range(tiles):
                fq = jnp.where(sub < 4, HQ[t, 2 * m : 2 * m + 1, :], HQ[t, 2 * m + 1 : 2 * m + 2, :])
                raw = rows_in[it, t, SUB * m : SUB * (m + 1), :]
                halos[m][t] = raw * (1.0 - fq) + jnp.where(head, fq, 0.0)
        for r, total in row_terms(halos):
            C[r] = total * rden_rows[r]
        for f in range(4):
            for r in range(R):
                into = Z.at[0, r] if f == 0 else state.at[f - 1, r]
                south, north = column_term(f, r)
                for t in range(tiles):
                    cut = slice(t * LANES, (t + 1) * LANES)
                    add = row_term(r, f, t)
                    if t == 0:
                        add = add + half_rden[r, :, cut] * south
                    if t == tiles - 1:
                        add = add + half_rden[r, :, cut] * north
                    into[:, cut] = into[:, cut] + add

        drain(stat_in.at[it, pl.ds(1, n - 1)], stat_send)
        drain(rows_out.at[it], row_send)
        drain(lat_in.at[it], slab_send)

        @pl.when(is_last)
        def _():
            drain(fold_in.at[it, pl.ds(0, nlon - 1)], slab_send)

        return carry

    lax.fori_loop(0, ITERS, iteration, 0)
    outputs = (damage_ref, stress_ref.at[0], stress_ref.at[1], stress_ref.at[2])
    for t in range(tiles):
        cut = slice(t * LANES, t * LANES + span[t])
        for k, target in enumerate(outputs):
            for r in range(R):
                value = Z[0, r, :, t * LANES : (t + 1) * LANES] if k == 0 else state[k - 1, r, :, t * LANES : (t + 1) * LANES]
                stage[k, t, pl.ds(r, SUB, stride=R), :] = value
            target[:, cut] = stage[k, t, :, : span[t]]


def write_out(stress_vmem, damage_vmem, mean_vmem, stress_hbm, damage_hbm, mean_hbm, mean_smem, sem):
    copies = [
        pltpu.make_async_copy(stress_vmem, stress_hbm, sem.at[0]),
        pltpu.make_async_copy(damage_vmem, damage_hbm, sem.at[1]),
        pltpu.make_async_copy(mean_smem, mean_hbm, sem.at[2]),
    ]
    copies[0].start()
    copies[1].start()
    row = mean_vmem[0:1, :]
    for k in range(ITERS):
        mean_smem[k] = row[0, k]
    copies[2].start()
    for copy in copies:
        copy.wait()


def shards(nlon, nlat, strain_rate, stress_start, concentration, cell_class, land_mask, fold_partner, kernel_weights):
    ncols, nrows = concentration.shape
    side = kernel_weights.shape[0]
    width = side // 2
    R = ncols // SUB
    L = -(-(nrows + 2 * width) // LANES) * LANES
    tiles = L // LANES
    n = nlon * nlat
    V = lambda *shape: pltpu.VMEM(shape, F32)
    S = lambda *shape: pltpu.SemaphoreType.DMA(shape)
    planes = R + 2 * width
    ext = -(-(ncols + 2 * width) // SUB) * SUB
    hbm = pl.BlockSpec(memory_space=pltpu.HBM)
    vmem = pl.BlockSpec(memory_space=pltpu.VMEM)
    stress, damage, mean = pl.pallas_call(
        functools.partial(kernel, nlon, nlat, nrows, R, L, side),
        out_shape=(
            pltpu.VMEM((3, ncols, nrows), F32),
            pltpu.VMEM((ncols, nrows), F32),
            pltpu.VMEM((SUB, LANES), F32),
        ),
        in_specs=[hbm] * 7,
        out_specs=(vmem,) * 3,
        scratch_shapes=[
            pltpu.SMEM(kernel_weights.shape, F32), pltpu.SMEM(fold_partner.shape, jnp.int32),
            pltpu.SMEM((ncols + 2 * width,), jnp.int32),
            V(9, R, SUB, L), V(9, R, SUB, L), V(planes, SUB, L),
            V(3, R, SUB, L), V(R, SUB, L), V(R, SUB, L), V(R, SUB, L), V(R, SUB, L), V(R, SUB, L), V(3, R, SUB, L),
            V(ITERS, tiles, SUB * width, LANES), V(ITERS, tiles, SUB * (width + 1), LANES),
            V(2, 2, 4, L), V(2, 2, 4, L), V(tiles, SUB, LANES), V(tiles, SUB, LANES),
            V(width * side, SUB, LANES), V(width * side, SUB, LANES), V(width, SUB, L), V(width, SUB, L),
            V(ITERS, 2, SUB, LANES), V(ITERS, 3, SUB, LANES), V(ITERS, nlon, SUB, LANES),
            V(nlon * R * SUB, LANES), V(ext, LANES), V(2, R, SUB, LANES),
            V(ITERS, 2, LANES), V(ITERS, n, 2, LANES), V(9, tiles, ncols, LANES),
            V(3, ncols, nrows), V(3, ncols, nrows), V(ncols, nrows),
            pltpu.VMEM((ncols, nrows), jnp.int32), pltpu.VMEM((ncols, nrows), jnp.int32),
            S(7), pltpu.SemaphoreType.DMA, pltpu.SemaphoreType.DMA, pltpu.SemaphoreType.DMA, S(ITERS),
            pltpu.SemaphoreType.DMA, S(ITERS), S(ITERS), pltpu.SemaphoreType.DMA, S(ITERS),
        ],
        compiler_params=pltpu.CompilerParams(
            collective_id=0, has_side_effects=True, vmem_limit_bytes=67043328 - 1024 * 1024
        ),
    )(kernel_weights, fold_partner, strain_rate, stress_start, concentration, cell_class, land_mask)
    return pl.pallas_call(
        write_out,
        out_shape=(
            jax.ShapeDtypeStruct((3, ncols, nrows), F32),
            jax.ShapeDtypeStruct((ncols, nrows), F32),
            jax.ShapeDtypeStruct((ITERS,), F32),
        ),
        in_specs=[vmem] * 3,
        out_specs=(hbm,) * 3,
        scratch_shapes=[pltpu.SMEM((ITERS,), F32), S(3)],
    )(stress, damage, mean)


def solution(mesh):
    in_specs = (
        P(None, "lon", "lat"),
        P(None, "lon", "lat"),
        P("lon", "lat"),
        P(("member", "lon"), "lat"),
        P("lon", "lat"),
        P(),
        P(),
    )
    out_specs = (P(None, ("member", "lon"), "lat"), P(("member", "lon"), "lat"), P("member"))
    body = functools.partial(shards, mesh.shape["lon"], mesh.shape["lat"])
    return jax.shard_map(body, mesh=mesh, in_specs=in_specs, out_specs=out_specs, check_vma=False)
```

```python
import functools

import jax
import jax.numpy as jnp
from jax import lax
from jax.experimental import pallas as pl
from jax.experimental.pallas import tpu as pltpu
from jax.sharding import PartitionSpec as P

ITERS = 3
LANES = 128
SUB = 8
NORTH = 66
MESH = pl.DeviceIdType.MESH
F32 = jnp.float32


def kernel(
    nlon, nlat, nrows, R, L, side,
    w_hbm, partner_hbm, e_hbm, s_hbm, conc_hbm, class_hbm, mask_hbm,
    stress_ref, damage_ref, mean_ref,
    w_ref, partner_ref, where_ref,
    Z, Y, X, load, base, ocean, orl, half_ocean, half_rden, state,
    rows_out, rows_in, fixed_out, fixed_in, fixed_rows, HQ, WR, WC, C, rden_rows,
    slab, lat_in, fold_in, tops, D, T, stat, stat_in, stage,
    e_ref, s_ref, conc_ref, class_ref, mask_ref,
    in_sem, fixed_send, fixed_recv, row_send, row_recv, slab_send, lat_recv, fold_recv, stat_send, stat_recv,
):
    width = side // 2
    n = nlon * nlat
    ncols = R * SUB
    tiles = L // LANES
    lon, lat = lax.axis_index("lon"), lax.axis_index("lat")
    member = lax.axis_index("member")
    is_last = lat == nlat - 1
    me = lon * nlat + lat
    nb = nrows - (L - LANES)

    def dev(a, b):
        return (member, a, b)

    def peer(d):
        other = lax.rem(me + d, n)
        return dev(other // nlat, lax.rem(other, nlat))

    def every(first, last, body):
        if last - first <= 16:
            for d in range(first, last):
                body(d)
        else:
            lax.fori_loop(first, last, lambda d, c: (body(d), c)[1], 0)

    def tile(x, t):
        return x[:, t * LANES : (t + 1) * LANES]

    right, left = lax.rem(lon + 1, nlon), lax.rem(lon + nlon - 1, nlon)
    other_lat = lax.rem(lat + 1, nlat)

    loads = [
        pltpu.make_async_copy(a, b, in_sem.at[k])
        for k, (a, b) in enumerate((
            (mask_hbm, mask_ref), (conc_hbm, conc_ref), (class_hbm, class_ref), (s_hbm, s_ref), (e_hbm, e_ref),
            (w_hbm, w_ref), (partner_hbm, partner_ref),
        ))
    ]
    for copy in loads:
        copy.start()
    barrier = pltpu.get_barrier_semaphore()
    every(1, n, lambda d: pl.semaphore_signal(barrier, inc=1, device_id=peer(d), device_id_type=MESH))

    sub = lax.broadcasted_iota(jnp.int32, (SUB, LANES), 0)
    sub_wide = lax.broadcasted_iota(jnp.int32, (SUB, L), 0)
    lane = lax.broadcasted_iota(jnp.int32, (SUB, LANES), 1)
    slot = lax.rem(lane, width)
    packed_slot = lax.rem(lax.rem(lane, 16), width)

    edge = jnp.zeros((SUB, LANES), F32)
    for r in range(R):
        for ref in (base.at[r], ocean.at[r], orl.at[r], *(load.at[k, r] for k in range(3)), Z.at[0, r],
                    *(state.at[k, r] for k in range(3))):
            ref[:, L - LANES :] = edge
    for t in range(tiles):
        for it in range(ITERS):
            rows_in[it, t, SUB * width :, :] = edge
        fixed_rows[t] = edge
    mean_ref[...] = edge
    for copy in loads[5:]:
        copy.wait()
    for d in range(width):
        for b in range(side):
            WR[d * side + b] = jnp.where(sub < 4, w_ref[d, b], w_ref[side - 1 - d, b])
    span_lanes = 5 * width
    for d in range(1, width + 1):
        keep = (slot >= width - d) & ((lane < span_lanes) | ((lane >= NORTH) & (lane < NORTH + span_lanes)))
        for a in range(side):
            WC[(d - 1) * side + a] = jnp.where(
                keep, jnp.where(lane < NORTH - width, w_ref[a, width - d], w_ref[a, width + d]), 0.0
            )
    for i in range(ncols + 2 * width):
        p = partner_ref[lax.rem(lon * ncols + i - width + nlon * ncols, nlon * ncols)]
        col = lax.rem(p, ncols)
        where_ref[i] = ((p // ncols) * R + lax.rem(col, R)) * SUB + col // R
    span = [min(LANES, nrows - t * LANES) for t in range(tiles)]

    def regroup(first, refs, t):
        cut = slice(t * LANES, t * LANES + span[t])
        for k, source in enumerate(refs):
            stage[first + k, t, :, : span[t]] = source[:, cut].astype(F32)
        for r in range(R):
            yield r, cut, [
                stage[first + k, t, pl.ds(r, SUB, stride=R), :][:, : span[t]] for k in range(len(refs))
            ]

    for copy in loads[:2]:
        copy.wait()
    count = jnp.zeros((SUB, LANES), F32)
    for t in range(tiles):
        for r, cut, (oc, conc) in regroup(0, (mask_ref, conc_ref), t):
            ocean[r, :, cut] = oc
            orl[r, :, cut] = oc / (0.6 * conc)
            base[r, :, cut] = conc * jnp.exp(-2.0 * (1.0 - conc))
            Z[0, r, :, cut] = oc * 0.1 * conc
    for m in range(width):
        fixed_out[0, 0, m : m + 1, :] = orl[R - width + m, SUB - 1 : SUB, :]
        fixed_out[0, 1, m : m + 1, :] = ocean[R - width + m, SUB - 1 : SUB, :]
        fixed_out[1, 0, m : m + 1, :] = orl[width - 1 - m, 0:1, :]
        fixed_out[1, 1, m : m + 1, :] = ocean[width - 1 - m, 0:1, :]

    def fixed_copy(k, to):
        return pltpu.make_async_remote_copy(
            src_ref=fixed_out.at[k, :, pl.ds(0, width), :], dst_ref=fixed_in.at[k, :, pl.ds(0, width), :],
            send_sem=fixed_send, recv_sem=fixed_recv, device_id=dev(to, lat), device_id_type=MESH,
        )

    def far_first(up, down):
        odd = lax.rem(lon, 2) == 1

        @pl.when(odd)
        def _():
            up()
            down()

        @pl.when(jnp.logical_not(odd))
        def _():
            down()
            up()

    for copy in loads[2:5]:
        copy.wait()
    sources = (class_ref, s_ref.at[0], s_ref.at[1], s_ref.at[2], e_ref.at[0], e_ref.at[1], e_ref.at[2])
    for t in range(tiles):
        for r, cut, (grade, s1, s2, s3, one, two, shear) in regroup(2, sources, t):
            oc = ocean[r, :, cut]
            Z[0, r, :, cut] = Z[0, r, :, cut] * grade
            for k, part in enumerate((s1, s2, s3)):
                state[k, r, :, cut] = oc * part
            load[0, r, :, cut] = (one + two / 3.0) / (8.0 / 9.0)
            load[1, r, :, cut] = (two + one / 3.0) / (8.0 / 9.0)
            load[2, r, :, cut] = (shear / (4.0 / 3.0)) / (8.0 / 9.0)
    for r in range(R):
        oc = ocean[r]
        Z[8, r] = oc
        half_ocean[r] = 0.5 * oc
        for t in range(tiles):
            count = count + tile(oc, t)
    count = jnp.sum(count, axis=0, keepdims=True)
    pl.semaphore_wait(barrier, n - 1)
    far_first(lambda: fixed_copy(0, right).start(), lambda: fixed_copy(1, left).start())

    def conv(f, c):
        for r in range(R):
            X[width + r] = Z[f, r]
        for m in range(width):
            X[m] = jnp.where(sub_wide == 0, 0.0, pltpu.roll(Z[f, m + R - width], 1, 0))
            X[R + width + m] = jnp.where(sub_wide == SUB - 1, 0.0, pltpu.roll(Z[f, m], SUB - 1, 0))
        for b in range(side):
            acc = [None] * R
            for p in range(R + 2 * width):
                x = X[p]
                for r in range(R):
                    a = p - r
                    if 0 <= a < side:
                        term = w_ref[a, b] * x
                        acc[r] = term if acc[r] is None else acc[r] + term
            for r in range(R):
                moved = acc[r] if b == width else pltpu.roll(acc[r], (width - b) % L, 1)
                if b == 0:
                    Y[f, r] = moved
                else:
                    Y[f, r] = Y[f, r] + moved
        return c

    def row_terms(halos):
        for r in range(width):
            total = None
            for b in range(side):
                parts = []
                for t in range(tiles):
                    acc = None
                    for m in range(r, width):
                        term = WR[(m - r) * side + b] * halos[m][t]
                        acc = term if acc is None else acc + term
                    parts.append(acc)
                wide = jnp.concatenate(parts, axis=1)
                wide = wide if b == width else pltpu.roll(wide, (width - b) % L, 1)
                total = wide if total is None else total + wide
            yield r, total

    def row_term(p, f, t):
        cut = slice(t * LANES, (t + 1) * LANES)
        out = jnp.zeros((SUB, LANES), F32)
        if p < width:
            out = jnp.where(sub == 0, C[p, f : f + 1, cut], out)
        if R - 1 - p < width:
            out = jnp.where(sub == SUB - 1, C[R - 1 - p, 4 + f : 5 + f, cut], out)
        return out

    def flip(x, at):
        y = jnp.where(at == 0, pltpu.roll(x, LANES - (width - 1), 1), x)
        return jnp.where(at == width - 1, pltpu.roll(x, width - 1, 1), y)

    def column_term(f, p):
        at = width * f + width
        south = jnp.where(lane < width, pltpu.roll(T[0, p], (LANES - at) % LANES, 1), 0.0)
        north = jnp.where(
            (lane >= nb - width) & (lane < nb), pltpu.roll(T[1, p], (nb - width - NORTH - at) % LANES, 1), 0.0
        )
        return south, north

    def iteration(it, carry):
        excess = jnp.zeros((SUB, LANES), F32)
        for r in range(R):
            oc = ocean[r]
            damage = Z[0, r]
            keep = 1.0 - damage
            square = keep * keep
            scale = oc * square / (square + 0.5)
            bk = base[r] * keep
            el = [scale * (state[k, r] + bk * load[k, r]) for k in range(3)]
            half = (el[0] - el[1]) * 0.5
            tau = jnp.sqrt(half * half + el[2] * el[2] + 0.25)
            over = jnp.maximum((tau + 0.35 * (el[0] + el[1])) * orl[r], 1.0)
            q = 1.0 - 1.0 / over
            for t in range(tiles):
                excess = excess + (tile(over, t) - 1.0)
            Z[4, r] = keep * q
            for k in range(3):
                Z[1 + k, r] = el[k]
                Z[5 + k, r] = el[k] * q
            for m in range(width):
                for f, part in enumerate((damage, *el)):
                    for t in range(tiles):
                        if r == R - width + m:
                            rows_out[it, t, SUB * m + f : SUB * m + f + 1, :] = tile(part, t)[SUB - 1 : SUB]
                        if r == width - 1 - m:
                            rows_out[it, t, SUB * m + 4 + f : SUB * m + 5 + f, :] = tile(part, t)[0:1]
        stat[it, 0:1, :] = jnp.sum(excess, axis=0, keepdims=True)
        stat[it, 1:2, :] = count

        def stat_copy(d):
            return pltpu.make_async_remote_copy(
                src_ref=stat.at[it], dst_ref=stat_in.at[it, d], send_sem=stat_send,
                recv_sem=stat_recv.at[it], device_id=peer(d), device_id_type=MESH,
            )

        def row_copy(s, m, to):
            piece = pl.ds(SUB * m + 4 * s, 4)
            return pltpu.make_async_remote_copy(
                src_ref=rows_out.at[it, :, piece, :], dst_ref=rows_in.at[it, :, piece, :], send_sem=row_send,
                recv_sem=row_recv.at[it], device_id=dev(to, lat), device_id_type=MESH,
            )

        def start_rows(s, to, ms):
            for m in ms:
                row_copy(s, m, to).start()

        every(1, n, lambda d: stat_copy(d).start())
        far_first(lambda: start_rows(0, right, [0]), lambda: start_rows(1, left, [0]))

        low = jnp.zeros((SUB, LANES), F32)
        high = jnp.zeros((SUB, LANES), F32)
        for r in range(R):
            for f in range(9):
                at = 32 * r + (width * f if f < 4 else (16 + width * (f - 4) if f < 8 else 4 * width))
                here = (lane >= at) & (lane < at + width)
                low = jnp.where(here, pltpu.roll(Z[f, r, :, :LANES], at, 1), low)
                high = jnp.where(here, pltpu.roll(Z[f, r, :, L - LANES :], (at + width - nb) % LANES, 1), high)
        slab[it, 0] = jnp.where(is_last, low, high)
        slab[it, 1] = high

        def lat_copy(k):
            to = lax.rem(lon + 1 - k + nlon, nlon)
            return pltpu.make_async_remote_copy(
                src_ref=slab.at[it, 0], dst_ref=lat_in.at[it, k], send_sem=slab_send,
                recv_sem=lat_recv.at[it], device_id=dev(to, other_lat), device_id_type=MESH,
            )

        def fold_copy(d):
            return pltpu.make_async_remote_copy(
                src_ref=slab.at[it, 1], dst_ref=fold_in.at[it, lon],
                send_sem=slab_send, recv_sem=fold_recv.at[it],
                device_id=dev(lax.rem(lon + d, nlon), lat), device_id_type=MESH,
            )

        @pl.when(is_last)
        def _():
            every(1, nlon, lambda d: fold_copy(d).start())
            fold_in[it, lon] = slab[it, 1]

        for k in range(3):
            lat_copy(k).start()

        rest = list(range(1, width))
        far_first(lambda: start_rows(0, right, rest), lambda: start_rows(1, left, rest))

        lax.fori_loop(0, jnp.where(it == 0, 9, 8), conv, 0)

        def drain(ref, sem):
            pltpu.make_async_copy(ref, ref, sem).wait()

        def wait_slabs():
            drain(lat_in.at[it], lat_recv.at[it])

            @pl.when(is_last)
            def _():
                drain(fold_in.at[it, pl.ds(0, nlon - 1)], fold_recv.at[it])

        drain(stat_in.at[it, pl.ds(1, n - 1)], stat_recv.at[it])
        total = stat[it]
        if n <= 16:
            for d in range(1, n):
                total = total + stat_in[it, d]
        else:
            total = lax.fori_loop(1, n, lambda d, c: c + stat_in[it, d], total)
        sums = jnp.sum(total, axis=1, keepdims=True)
        mean = sums[0:1] / (sums[1:2] + 1.0)
        factor = 1.0 / (1.0 + 2.0 * mean)
        mean_ref[...] = jnp.where(lane == it, mean, mean_ref[...])

        def columns():
            signed = jnp.where(lax.rem(lane, 32) < width, factor, -factor)

            @pl.when(is_last)
            def _():
                def spread(k):
                    got = fold_in[it, k]
                    got = got + signed * pltpu.roll(got, LANES - 16, 1)
                    for r in range(R):
                        tops[pl.ds((k * R + r) * SUB, SUB), :] = pltpu.roll(got, (NORTH - 32 * r) % LANES, 1)

                every(0, nlon, spread)
                for i in range(ncols + 2 * width):
                    D[i : i + 1, :] = tops[pl.ds(where_ref[i], 1), :]

            south_side = lane < NORTH - width
            own = []
            for k in range(3):
                got = lat_in[it, k]
                got = got + signed * pltpu.roll(got, LANES - 16, 1)
                own.append(jnp.where(is_last, got, flip(got, packed_slot)))

            def piece(k, r):
                return jnp.where(
                    is_last, pltpu.roll(own[k], (LANES - 32 * r) % LANES, 1),
                    pltpu.roll(own[k], (NORTH - 32 * r) % LANES, 1),
                )

            mid = [piece(1, r) for r in range(R)]
            ghosts = [None] * (R + 2 * width)
            for r in range(R):
                ghosts[width + r] = mid[r]
            for m in range(width):
                r = m + R - width
                ghosts[m] = jnp.where(sub == 0, pltpu.roll(piece(0, r), 1, 0), pltpu.roll(mid[r], 1, 0))
                ghosts[R + width + m] = jnp.where(
                    sub == SUB - 1, pltpu.roll(piece(2, m), SUB - 1, 0), pltpu.roll(mid[m], SUB - 1, 0)
                )
            for p in range(R + 2 * width):
                fold = D[pl.ds(p, SUB, stride=R), :]
                ghosts[p] = jnp.where(
                    south_side, jnp.where(is_last, ghosts[p], 0.0), jnp.where(is_last, fold, ghosts[p])
                )
            for r in range(R):
                total = None
                for d in range(1, width + 1):
                    acc = None
                    for a in range(side):
                        term = WC[(d - 1) * side + a] * ghosts[r + a]
                        acc = term if acc is None else acc + term
                    acc = pltpu.roll(acc, d, 1)
                    total = acc if total is None else total + acc
                T[0, r] = total
                T[1, r] = flip(total, slot)

        def finish_ocean():
            drain(fixed_in.at[:, :, pl.ds(0, width), :], fixed_recv)
            drain(fixed_in.at[:, :, pl.ds(0, width), :], fixed_send)
            for t in range(tiles):
                cut = slice(t * LANES, (t + 1) * LANES)
                for m in range(width):
                    for s in range(2):
                        fixed_rows[t, 2 * m + s : 2 * m + s + 1, :] = fixed_in[s, 0, m : m + 1, cut]
            halos = [
                [
                    jnp.where(
                        sub < 4, fixed_in[0, 1, m : m + 1, t * LANES : (t + 1) * LANES],
                        fixed_in[1, 1, m : m + 1, t * LANES : (t + 1) * LANES],
                    )
                    for t in range(tiles)
                ]
                for m in range(width)
            ]
            for r, total in row_terms(halos):
                C[r] = total
            for r in range(R):
                south, north = column_term(4, r)
                for t in range(tiles):
                    cut = slice(t * LANES, (t + 1) * LANES)
                    denom = Y[8, r, :, cut] + row_term(r, 0, t)
                    if t == 0:
                        denom = denom + south
                    if t == tiles - 1:
                        denom = denom + north
                    half_rden[r, :, cut] = half_ocean[r, :, cut] / (denom + 1.0)
            for r in range(width):
                rden_rows[r] = jnp.where(
                    sub_wide < 4, half_rden[r, 0:1, :], half_rden[R - 1 - r, SUB - 1 : SUB, :]
                )

        @pl.when(it == 0)
        def _():
            wait_slabs()
            columns()
            finish_ocean()

        for r in range(R):
            for t in range(tiles):
                cut = slice(t * LANES, (t + 1) * LANES)
                ho, hr = half_ocean[r, :, cut], half_rden[r, :, cut]
                for f in range(4):
                    part = factor if f == 0 else -factor
                    local = Z[f, r, :, cut] + part * Z[4 + f, r, :, cut]
                    spread_out = Y[f, r, :, cut] + part * Y[4 + f, r, :, cut]
                    fresh = ho * local + hr * spread_out
                    if f == 0:
                        Z[0, r, :, cut] = fresh
                    else:
                        state[f - 1, r, :, cut] = fresh

        @pl.when(it > 0)
        def _():
            wait_slabs()
            columns()

        for f in range(4):
            for r in range(R):
                into = Z.at[0, r] if f == 0 else state.at[f - 1, r]
                south, north = column_term(f, r)
                for t, term in ((0, south), (tiles - 1, north)):
                    cut = slice(t * LANES, (t + 1) * LANES)
                    into[:, cut] = into[:, cut] + half_rden[r, :, cut] * term

        drain(rows_in.at[it, :, pl.ds(0, SUB * width), :], row_recv.at[it])
        for t in range(tiles):
            e = [rows_in[it, t, pl.ds(k, SUB, stride=4), :] for k in range(1, 4)]
            half = (e[0] - e[1]) * 0.5
            tau = jnp.sqrt(half * half + e[2] * e[2] + 0.25)
            over = jnp.maximum((tau + 0.35 * (e[0] + e[1])) * fixed_rows[t], 1.0)
            HQ[t] = factor * (1.0 - 1.0 / over)
        halos = [[None] * tiles for _ in range(width)]
        head = (sub == 0) | (sub == 4)
        for m in range(width):
            for t in range(tiles):
                fq = jnp.where(sub < 4, HQ[t, 2 * m : 2 * m + 1, :], HQ[t, 2 * m + 1 : 2 * m + 2, :])
                raw = rows_in[it, t, SUB * m : SUB * (m + 1), :]
                halos[m][t] = raw * (1.0 - fq) + jnp.where(head, fq, 0.0)
        for r, total in row_terms(halos):
            C[r] = total * rden_rows[r]
        for f in range(4):
            for r in range(R):
                into = Z.at[0, r] if f == 0 else state.at[f - 1, r]
                for t in range(tiles):
                    cut = slice(t * LANES, (t + 1) * LANES)
                    into[:, cut] = into[:, cut] + row_term(r, f, t)

        drain(stat_in.at[it, pl.ds(1, n - 1)], stat_send)
        drain(rows_out.at[it], row_send)
        drain(lat_in.at[it], slab_send)

        @pl.when(is_last)
        def _():
            drain(fold_in.at[it, pl.ds(0, nlon - 1)], slab_send)

        return carry

    lax.fori_loop(0, ITERS, iteration, 0)
    outputs = (damage_ref, stress_ref.at[0], stress_ref.at[1], stress_ref.at[2])
    for t in range(tiles):
        cut = slice(t * LANES, t * LANES + span[t])
        for k, target in enumerate(outputs):
            for r in range(R):
                value = Z[0, r, :, t * LANES : (t + 1) * LANES] if k == 0 else state[k - 1, r, :, t * LANES : (t + 1) * LANES]
                stage[k, t, pl.ds(r, SUB, stride=R), :] = value
            target[:, cut] = stage[k, t, :, : span[t]]


def write_out(stress_vmem, damage_vmem, mean_vmem, stress_hbm, damage_hbm, mean_hbm, mean_smem, sem):
    copies = [
        pltpu.make_async_copy(stress_vmem, stress_hbm, sem.at[0]),
        pltpu.make_async_copy(damage_vmem, damage_hbm, sem.at[1]),
        pltpu.make_async_copy(mean_smem, mean_hbm, sem.at[2]),
    ]
    copies[0].start()
    copies[1].start()
    row = mean_vmem[0:1, :]
    for k in range(ITERS):
        mean_smem[k] = row[0, k]
    copies[2].start()
    for copy in copies:
        copy.wait()


def shards(nlon, nlat, strain_rate, stress_start, concentration, cell_class, land_mask, fold_partner, kernel_weights):
    ncols, nrows = concentration.shape
    side = kernel_weights.shape[0]
    width = side // 2
    R = ncols // SUB
    L = -(-(nrows + 2 * width) // LANES) * LANES
    tiles = L // LANES
    n = nlon * nlat
    V = lambda *shape: pltpu.VMEM(shape, F32)
    S = lambda *shape: pltpu.SemaphoreType.DMA(shape)
    planes = R + 2 * width
    ext = -(-(ncols + 2 * width) // SUB) * SUB
    hbm = pl.BlockSpec(memory_space=pltpu.HBM)
    vmem = pl.BlockSpec(memory_space=pltpu.VMEM)
    stress, damage, mean = pl.pallas_call(
        functools.partial(kernel, nlon, nlat, nrows, R, L, side),
        out_shape=(
            pltpu.VMEM((3, ncols, nrows), F32),
            pltpu.VMEM((ncols, nrows), F32),
            pltpu.VMEM((SUB, LANES), F32),
        ),
        in_specs=[hbm] * 7,
        out_specs=(vmem,) * 3,
        scratch_shapes=[
            pltpu.SMEM(kernel_weights.shape, F32), pltpu.SMEM(fold_partner.shape, jnp.int32),
            pltpu.SMEM((ncols + 2 * width,), jnp.int32),
            V(9, R, SUB, L), V(9, R, SUB, L), V(planes, SUB, L),
            V(3, R, SUB, L), V(R, SUB, L), V(R, SUB, L), V(R, SUB, L), V(R, SUB, L), V(R, SUB, L), V(3, R, SUB, L),
            V(ITERS, tiles, SUB * width, LANES), V(ITERS, tiles, SUB * (width + 1), LANES),
            V(2, 2, 4, L), V(2, 2, 4, L), V(tiles, SUB, LANES), V(tiles, SUB, LANES),
            V(width * side, SUB, LANES), V(width * side, SUB, LANES), V(width, SUB, L), V(width, SUB, L),
            V(ITERS, 2, SUB, LANES), V(ITERS, 3, SUB, LANES), V(ITERS, nlon, SUB, LANES),
            V(nlon * R * SUB, LANES), V(ext, LANES), V(2, R, SUB, LANES),
            V(ITERS, 2, LANES), V(ITERS, n, 2, LANES), V(9, tiles, ncols, LANES),
            V(3, ncols, nrows), V(3, ncols, nrows), V(ncols, nrows),
            pltpu.VMEM((ncols, nrows), jnp.int32), pltpu.VMEM((ncols, nrows), jnp.int32),
            S(7), pltpu.SemaphoreType.DMA, pltpu.SemaphoreType.DMA, pltpu.SemaphoreType.DMA, S(ITERS),
            pltpu.SemaphoreType.DMA, S(ITERS), S(ITERS), pltpu.SemaphoreType.DMA, S(ITERS),
        ],
        compiler_params=pltpu.CompilerParams(
            collective_id=0, has_side_effects=True, vmem_limit_bytes=67043328 - 1024 * 1024
        ),
    )(kernel_weights, fold_partner, strain_rate, stress_start, concentration, cell_class, land_mask)
    return pl.pallas_call(
        write_out,
        out_shape=(
            jax.ShapeDtypeStruct((3, ncols, nrows), F32),
            jax.ShapeDtypeStruct((ncols, nrows), F32),
            jax.ShapeDtypeStruct((ITERS,), F32),
        ),
        in_specs=[vmem] * 3,
        out_specs=(hbm,) * 3,
        scratch_shapes=[pltpu.SMEM((ITERS,), F32), S(3)],
    )(*(pltpu.with_memory_space_constraint(x, pltpu.VMEM) for x in (stress, damage, mean)))


def solution(mesh):
    in_specs = (
        P(None, "lon", "lat"),
        P(None, "lon", "lat"),
        P("lon", "lat"),
        P(("member", "lon"), "lat"),
        P("lon", "lat"),
        P(),
        P(),
    )
    out_specs = (P(None, ("member", "lon"), "lat"), P(("member", "lon"), "lat"), P("member"))
    body = functools.partial(shards, mesh.shape["lon"], mesh.shape["lat"])
    return jax.shard_map(body, mesh=mesh, in_specs=in_specs, out_specs=out_specs, check_vma=False)
```

```python
import functools

import jax
import jax.numpy as jnp
from jax import lax
from jax.experimental import pallas as pl
from jax.experimental.pallas import tpu as pltpu
from jax.sharding import PartitionSpec as P

ITERS = 3
LANES = 128
SUB = 8
NORTH = 66
MESH = pl.DeviceIdType.MESH
F32 = jnp.float32


def kernel(
    nlon, nlat, nrows, R, L, side,
    w_hbm, partner_hbm, e_hbm, s_hbm, conc_hbm, class_hbm, mask_hbm,
    stress_ref, damage_ref, mean_ref,
    w_ref, partner_ref, where_ref,
    Z, Y, XH, XL, TH, TL, load, base, ocean, orl, half_ocean, half_rden, state,
    rows_out, rows_in, fixed_out, fixed_in, fixed_rows, HQ, WR, WC, C, rden_rows,
    slab, lat_in, fold_in, tops, D, T, stat, stat_in, stage,
    e_ref, s_ref, conc_ref, class_ref, mask_ref,
    in_sem, fixed_send, fixed_recv, row_send, row_recv, slab_send, lat_recv, fold_recv, stat_send, stat_recv,
):
    width = side // 2
    n = nlon * nlat
    ncols = R * SUB
    tiles = L // LANES
    lon, lat = lax.axis_index("lon"), lax.axis_index("lat")
    member = lax.axis_index("member")
    is_last = lat == nlat - 1
    me = lon * nlat + lat
    nb = nrows - (L - LANES)

    def dev(a, b):
        return (member, a, b)

    def peer(d):
        other = lax.rem(me + d, n)
        return dev(other // nlat, lax.rem(other, nlat))

    def every(first, last, body):
        if last - first <= 16:
            for d in range(first, last):
                body(d)
        else:
            lax.fori_loop(first, last, lambda d, c: (body(d), c)[1], 0)

    def tile(x, t):
        return x[:, t * LANES : (t + 1) * LANES]

    right, left = lax.rem(lon + 1, nlon), lax.rem(lon + nlon - 1, nlon)
    other_lat = lax.rem(lat + 1, nlat)

    loads = [
        pltpu.make_async_copy(a, b, in_sem.at[k])
        for k, (a, b) in enumerate((
            (mask_hbm, mask_ref), (conc_hbm, conc_ref), (class_hbm, class_ref), (s_hbm, s_ref), (e_hbm, e_ref),
            (w_hbm, w_ref), (partner_hbm, partner_ref),
        ))
    ]
    for copy in loads:
        copy.start()
    barrier = pltpu.get_barrier_semaphore()
    every(1, n, lambda d: pl.semaphore_signal(barrier, inc=1, device_id=peer(d), device_id_type=MESH))

    sub = lax.broadcasted_iota(jnp.int32, (SUB, LANES), 0)
    sub_wide = lax.broadcasted_iota(jnp.int32, (SUB, L), 0)
    lane = lax.broadcasted_iota(jnp.int32, (SUB, LANES), 1)
    slot = lax.rem(lane, width)
    packed_slot = lax.rem(lax.rem(lane, 16), width)

    edge = jnp.zeros((SUB, LANES), F32)
    for r in range(R):
        for ref in (base.at[r], ocean.at[r], orl.at[r], *(load.at[k, r] for k in range(3)), Z.at[0, r],
                    *(state.at[k, r] for k in range(3))):
            ref[:, L - LANES :] = edge
    for t in range(tiles):
        for it in range(ITERS):
            rows_in[it, t, SUB * width :, :] = edge
        fixed_rows[t] = edge
    mean_ref[...] = edge
    for copy in loads[5:]:
        copy.wait()
    for d in range(width):
        for b in range(side):
            WR[d * side + b] = jnp.where(sub < 4, w_ref[d, b], w_ref[side - 1 - d, b])
    span_lanes = 5 * width
    for d in range(1, width + 1):
        keep = (slot >= width - d) & ((lane < span_lanes) | ((lane >= NORTH) & (lane < NORTH + span_lanes)))
        for a in range(side):
            WC[(d - 1) * side + a] = jnp.where(
                keep, jnp.where(lane < NORTH - width, w_ref[a, width - d], w_ref[a, width + d]), 0.0
            )
    for i in range(ncols + 2 * width):
        p = partner_ref[lax.rem(lon * ncols + i - width + nlon * ncols, nlon * ncols)]
        col = lax.rem(p, ncols)
        where_ref[i] = ((p // ncols) * R + lax.rem(col, R)) * SUB + col // R
    span = [min(LANES, nrows - t * LANES) for t in range(tiles)]

    def regroup(first, refs, t):
        cut = slice(t * LANES, t * LANES + span[t])
        for k, source in enumerate(refs):
            stage[first + k, t, :, : span[t]] = source[:, cut].astype(F32)
        for r in range(R):
            yield r, cut, [
                stage[first + k, t, pl.ds(r, SUB, stride=R), :][:, : span[t]] for k in range(len(refs))
            ]

    for copy in loads[:2]:
        copy.wait()
    count = jnp.zeros((SUB, LANES), F32)
    for t in range(tiles):
        for r, cut, (oc, conc) in regroup(0, (mask_ref, conc_ref), t):
            ocean[r, :, cut] = oc
            orl[r, :, cut] = oc / (0.6 * conc)
            base[r, :, cut] = conc * jnp.exp(-2.0 * (1.0 - conc))
            Z[0, r, :, cut] = oc * 0.1 * conc
    for m in range(width):
        fixed_out[0, 0, m : m + 1, :] = orl[R - width + m, SUB - 1 : SUB, :]
        fixed_out[0, 1, m : m + 1, :] = ocean[R - width + m, SUB - 1 : SUB, :]
        fixed_out[1, 0, m : m + 1, :] = orl[width - 1 - m, 0:1, :]
        fixed_out[1, 1, m : m + 1, :] = ocean[width - 1 - m, 0:1, :]

    def fixed_copy(k, to):
        return pltpu.make_async_remote_copy(
            src_ref=fixed_out.at[k, :, pl.ds(0, width), :], dst_ref=fixed_in.at[k, :, pl.ds(0, width), :],
            send_sem=fixed_send, recv_sem=fixed_recv, device_id=dev(to, lat), device_id_type=MESH,
        )

    def far_first(up, down):
        odd = lax.rem(lon, 2) == 1

        @pl.when(odd)
        def _():
            up()
            down()

        @pl.when(jnp.logical_not(odd))
        def _():
            down()
            up()

    for copy in loads[2:5]:
        copy.wait()
    sources = (class_ref, s_ref.at[0], s_ref.at[1], s_ref.at[2], e_ref.at[0], e_ref.at[1], e_ref.at[2])
    for t in range(tiles):
        for r, cut, (grade, s1, s2, s3, one, two, shear) in regroup(2, sources, t):
            oc = ocean[r, :, cut]
            Z[0, r, :, cut] = Z[0, r, :, cut] * grade
            for k, part in enumerate((s1, s2, s3)):
                state[k, r, :, cut] = oc * part
            load[0, r, :, cut] = (one + two / 3.0) / (8.0 / 9.0)
            load[1, r, :, cut] = (two + one / 3.0) / (8.0 / 9.0)
            load[2, r, :, cut] = (shear / (4.0 / 3.0)) / (8.0 / 9.0)
    for r in range(R):
        oc = ocean[r]
        Z[8, r] = oc
        Z[9, r] = jnp.zeros((SUB, L), F32)
        half_ocean[r] = 0.5 * oc
        for t in range(tiles):
            count = count + tile(oc, t)
    count = jnp.sum(count, axis=0, keepdims=True)
    pl.semaphore_wait(barrier, n - 1)
    far_first(lambda: fixed_copy(0, right).start(), lambda: fixed_copy(1, left).start())

    pairs = (R + 2 * width) // 2
    taps = (side + 1) // 2
    step = LANES - 2 * width
    block = 2 * tiles * SUB

    def build_bands():
        for strip in range(LANES // 16):
            row = lax.broadcasted_iota(jnp.int32, (16, LANES), 0)
            offset = row + 16 * strip + width - lax.broadcasted_iota(jnp.int32, (16, LANES), 1)
            hits = [offset == b for b in range(side)]
            for a in range(-1, side + 1):
                band = jnp.zeros((16, LANES), F32)
                if 0 <= a < side:
                    for b in range(side):
                        band = jnp.where(hits[b], w_ref[a, b], band)
                high = band.astype(jnp.bfloat16)
                low = (band - high.astype(F32)).astype(jnp.bfloat16)
                for k in range(taps):
                    for u in range(2):
                        for v in range(2):
                            if 2 * k + u - v == a:
                                at = (slice(k * 256 + u * LANES + 16 * strip, k * 256 + u * LANES + 16 * strip + 16),
                                      slice(v * LANES, (v + 1) * LANES))
                                TH[at] = high
                                TL[at] = low

    def conv(g, c):
        chunks = []
        for r in range(R):
            plane = []
            for i in range(2):
                last = None
                for t in range(tiles):
                    shift = width + (LANES - step) * t
                    here = Z[2 * g + i, r, :, t * LANES : (t + 1) * LANES]
                    now = pltpu.roll(here, shift, 1)
                    before = 0.0 if last is None else pltpu.roll(last, shift, 1)
                    plane.append(jnp.where(lane < shift, before, now))
                    last = here
            chunks.append(plane)
        for p in range(R + 2 * width):
            if p < width:
                plane = [jnp.where(sub == 0, 0.0, pltpu.roll(x, 1, 0)) for x in chunks[p + R - width]]
            elif p < width + R:
                plane = chunks[p - width]
            else:
                plane = [jnp.where(sub == SUB - 1, 0.0, pltpu.roll(x, SUB - 1, 0)) for x in chunks[p - width - R]]
            for j in range(tiles):
                x = jnp.concatenate(plane[2 * j : 2 * j + 2], axis=0)
                high = x.astype(jnp.bfloat16)
                at = (slice((p // 2) * block + 16 * j, (p // 2) * block + 16 * j + 16),
                      slice((p % 2) * LANES, (p % 2 + 1) * LANES))
                XH[at] = high
                XL[at] = (x - high.astype(F32)).astype(jnp.bfloat16)
        out = None
        for k in range(taps):
            rows = slice(k * block, k * block + (R // 2) * block)
            band = slice(k * 256, (k + 1) * 256)
            for x, w in ((XH, TH), (XL, TH), (XH, TL)):
                term = jnp.dot(x[rows, :], w[band, :], preferred_element_type=F32)
                out = term if out is None else out + term
        for r in range(R):
            for i in range(2):
                def part(t):
                    row = (r // 2) * block + (i * tiles + t) * SUB
                    return out[row : row + SUB, (r % 2) * LANES : (r % 2 + 1) * LANES]
                for t in range(tiles):
                    first = width + (LANES - step) * t
                    value = pltpu.roll(part(t), LANES - first, 1)
                    if t + 1 < tiles:
                        rest = pltpu.roll(part(t + 1), LANES - width - first - width, 1)
                        value = jnp.where(lane < LANES - width - first, value, rest)
                    Y[2 * g + i, r, :, t * LANES : (t + 1) * LANES] = value
        return c

    def row_terms(halos):
        for r in range(width):
            total = None
            for b in range(side):
                parts = []
                for t in range(tiles):
                    acc = None
                    for m in range(r, width):
                        term = WR[(m - r) * side + b] * halos[m][t]
                        acc = term if acc is None else acc + term
                    parts.append(acc)
                wide = jnp.concatenate(parts, axis=1)
                wide = wide if b == width else pltpu.roll(wide, (width - b) % L, 1)
                total = wide if total is None else total + wide
            yield r, total

    def row_term(p, f, t):
        cut = slice(t * LANES, (t + 1) * LANES)
        out = jnp.zeros((SUB, LANES), F32)
        if p < width:
            out = jnp.where(sub == 0, C[p, f : f + 1, cut], out)
        if R - 1 - p < width:
            out = jnp.where(sub == SUB - 1, C[R - 1 - p, 4 + f : 5 + f, cut], out)
        return out

    def flip(x, at):
        y = jnp.where(at == 0, pltpu.roll(x, LANES - (width - 1), 1), x)
        return jnp.where(at == width - 1, pltpu.roll(x, width - 1, 1), y)

    def column_term(f, p):
        at = width * f + width
        south = jnp.where(lane < width, pltpu.roll(T[0, p], (LANES - at) % LANES, 1), 0.0)
        north = jnp.where(
            (lane >= nb - width) & (lane < nb), pltpu.roll(T[1, p], (nb - width - NORTH - at) % LANES, 1), 0.0
        )
        return south, north

    def iteration(it, carry):
        excess = jnp.zeros((SUB, LANES), F32)
        for r in range(R):
            oc = ocean[r]
            damage = Z[0, r]
            keep = 1.0 - damage
            square = keep * keep
            scale = oc * square / (square + 0.5)
            bk = base[r] * keep
            el = [scale * (state[k, r] + bk * load[k, r]) for k in range(3)]
            half = (el[0] - el[1]) * 0.5
            tau = jnp.sqrt(half * half + el[2] * el[2] + 0.25)
            over = jnp.maximum((tau + 0.35 * (el[0] + el[1])) * orl[r], 1.0)
            q = 1.0 - 1.0 / over
            for t in range(tiles):
                excess = excess + (tile(over, t) - 1.0)
            Z[4, r] = keep * q
            for k in range(3):
                Z[1 + k, r] = el[k]
                Z[5 + k, r] = el[k] * q
            for m in range(width):
                for f, part in enumerate((damage, *el)):
                    for t in range(tiles):
                        if r == R - width + m:
                            rows_out[it, t, SUB * m + f : SUB * m + f + 1, :] = tile(part, t)[SUB - 1 : SUB]
                        if r == width - 1 - m:
                            rows_out[it, t, SUB * m + 4 + f : SUB * m + 5 + f, :] = tile(part, t)[0:1]
        stat[it, 0:1, :] = jnp.sum(excess, axis=0, keepdims=True)
        stat[it, 1:2, :] = count

        def stat_copy(d):
            return pltpu.make_async_remote_copy(
                src_ref=stat.at[it], dst_ref=stat_in.at[it, d], send_sem=stat_send,
                recv_sem=stat_recv.at[it], device_id=peer(d), device_id_type=MESH,
            )

        def row_copy(s, m, to):
            piece = pl.ds(SUB * m + 4 * s, 4)
            return pltpu.make_async_remote_copy(
                src_ref=rows_out.at[it, :, piece, :], dst_ref=rows_in.at[it, :, piece, :], send_sem=row_send,
                recv_sem=row_recv.at[it], device_id=dev(to, lat), device_id_type=MESH,
            )

        def start_rows(s, to, ms):
            for m in ms:
                row_copy(s, m, to).start()

        every(1, n, lambda d: stat_copy(d).start())
        far_first(lambda: start_rows(0, right, [0]), lambda: start_rows(1, left, [0]))

        low = jnp.zeros((SUB, LANES), F32)
        high = jnp.zeros((SUB, LANES), F32)
        for r in range(R):
            for f in range(9):
                at = 32 * r + (width * f if f < 4 else (16 + width * (f - 4) if f < 8 else 4 * width))
                here = (lane >= at) & (lane < at + width)
                low = jnp.where(here, pltpu.roll(Z[f, r, :, :LANES], at, 1), low)
                high = jnp.where(here, pltpu.roll(Z[f, r, :, L - LANES :], (at + width - nb) % LANES, 1), high)
        slab[it, 0] = jnp.where(is_last, low, high)
        slab[it, 1] = high

        def lat_copy(k):
            to = lax.rem(lon + 1 - k + nlon, nlon)
            return pltpu.make_async_remote_copy(
                src_ref=slab.at[it, 0], dst_ref=lat_in.at[it, k], send_sem=slab_send,
                recv_sem=lat_recv.at[it], device_id=dev(to, other_lat), device_id_type=MESH,
            )

        def fold_copy(d):
            return pltpu.make_async_remote_copy(
                src_ref=slab.at[it, 1], dst_ref=fold_in.at[it, lon],
                send_sem=slab_send, recv_sem=fold_recv.at[it],
                device_id=dev(lax.rem(lon + d, nlon), lat), device_id_type=MESH,
            )

        @pl.when(is_last)
        def _():
            every(1, nlon, lambda d: fold_copy(d).start())
            fold_in[it, lon] = slab[it, 1]

        for k in range(3):
            lat_copy(k).start()

        rest = list(range(1, width))
        far_first(lambda: start_rows(0, right, rest), lambda: start_rows(1, left, rest))

        @pl.when(it == 0)
        def _():
            build_bands()

        lax.fori_loop(0, jnp.where(it == 0, 5, 4), conv, 0)

        def drain(ref, sem):
            pltpu.make_async_copy(ref, ref, sem).wait()

        def wait_slabs():
            drain(lat_in.at[it], lat_recv.at[it])

            @pl.when(is_last)
            def _():
                drain(fold_in.at[it, pl.ds(0, nlon - 1)], fold_recv.at[it])

        drain(stat_in.at[it, pl.ds(1, n - 1)], stat_recv.at[it])
        total = stat[it]
        if n <= 16:
            for d in range(1, n):
                total = total + stat_in[it, d]
        else:
            total = lax.fori_loop(1, n, lambda d, c: c + stat_in[it, d], total)
        sums = jnp.sum(total, axis=1, keepdims=True)
        mean = sums[0:1] / (sums[1:2] + 1.0)
        factor = 1.0 / (1.0 + 2.0 * mean)
        mean_ref[...] = jnp.where(lane == it, mean, mean_ref[...])

        def columns():
            signed = jnp.where(lax.rem(lane, 32) < width, factor, -factor)

            @pl.when(is_last)
            def _():
                def spread(k):
                    got = fold_in[it, k]
                    got = got + signed * pltpu.roll(got, LANES - 16, 1)
                    for r in range(R):
                        tops[pl.ds((k * R + r) * SUB, SUB), :] = pltpu.roll(got, (NORTH - 32 * r) % LANES, 1)

                every(0, nlon, spread)
                for i in range(ncols + 2 * width):
                    D[i : i + 1, :] = tops[pl.ds(where_ref[i], 1), :]

            south_side = lane < NORTH - width
            own = []
            for k in range(3):
                got = lat_in[it, k]
                got = got + signed * pltpu.roll(got, LANES - 16, 1)
                own.append(jnp.where(is_last, got, flip(got, packed_slot)))

            def piece(k, r):
                return jnp.where(
                    is_last, pltpu.roll(own[k], (LANES - 32 * r) % LANES, 1),
                    pltpu.roll(own[k], (NORTH - 32 * r) % LANES, 1),
                )

            mid = [piece(1, r) for r in range(R)]
            ghosts = [None] * (R + 2 * width)
            for r in range(R):
                ghosts[width + r] = mid[r]
            for m in range(width):
                r = m + R - width
                ghosts[m] = jnp.where(sub == 0, pltpu.roll(piece(0, r), 1, 0), pltpu.roll(mid[r], 1, 0))
                ghosts[R + width + m] = jnp.where(
                    sub == SUB - 1, pltpu.roll(piece(2, m), SUB - 1, 0), pltpu.roll(mid[m], SUB - 1, 0)
                )
            for p in range(R + 2 * width):
                fold = D[pl.ds(p, SUB, stride=R), :]
                ghosts[p] = jnp.where(
                    south_side, jnp.where(is_last, ghosts[p], 0.0), jnp.where(is_last, fold, ghosts[p])
                )
            for r in range(R):
                total = None
                for d in range(1, width + 1):
                    acc = None
                    for a in range(side):
                        term = WC[(d - 1) * side + a] * ghosts[r + a]
                        acc = term if acc is None else acc + term
                    acc = pltpu.roll(acc, d, 1)
                    total = acc if total is None else total + acc
                T[0, r] = total
                T[1, r] = flip(total, slot)

        def finish_ocean():
            drain(fixed_in.at[:, :, pl.ds(0, width), :], fixed_recv)
            drain(fixed_in.at[:, :, pl.ds(0, width), :], fixed_send)
            for t in range(tiles):
                cut = slice(t * LANES, (t + 1) * LANES)
                for m in range(width):
                    for s in range(2):
                        fixed_rows[t, 2 * m + s : 2 * m + s + 1, :] = fixed_in[s, 0, m : m + 1, cut]
            halos = [
                [
                    jnp.where(
                        sub < 4, fixed_in[0, 1, m : m + 1, t * LANES : (t + 1) * LANES],
                        fixed_in[1, 1, m : m + 1, t * LANES : (t + 1) * LANES],
                    )
                    for t in range(tiles)
                ]
                for m in range(width)
            ]
            for r, total in row_terms(halos):
                C[r] = total
            for r in range(R):
                south, north = column_term(4, r)
                for t in range(tiles):
                    cut = slice(t * LANES, (t + 1) * LANES)
                    denom = Y[8, r, :, cut] + row_term(r, 0, t)
                    if t == 0:
                        denom = denom + south
                    if t == tiles - 1:
                        denom = denom + north
                    half_rden[r, :, cut] = half_ocean[r, :, cut] / (denom + 1.0)
            for r in range(width):
                rden_rows[r] = jnp.where(
                    sub_wide < 4, half_rden[r, 0:1, :], half_rden[R - 1 - r, SUB - 1 : SUB, :]
                )

        @pl.when(it == 0)
        def _():
            wait_slabs()
            columns()
            finish_ocean()

        for r in range(R):
            for t in range(tiles):
                cut = slice(t * LANES, (t + 1) * LANES)
                ho, hr = half_ocean[r, :, cut], half_rden[r, :, cut]
                for f in range(4):
                    part = factor if f == 0 else -factor
                    local = Z[f, r, :, cut] + part * Z[4 + f, r, :, cut]
                    spread_out = Y[f, r, :, cut] + part * Y[4 + f, r, :, cut]
                    fresh = ho * local + hr * spread_out
                    if f == 0:
                        Z[0, r, :, cut] = fresh
                    else:
                        state[f - 1, r, :, cut] = fresh

        @pl.when(it > 0)
        def _():
            wait_slabs()
            columns()

        for f in range(4):
            for r in range(R):
                into = Z.at[0, r] if f == 0 else state.at[f - 1, r]
                south, north = column_term(f, r)
                for t, term in ((0, south), (tiles - 1, north)):
                    cut = slice(t * LANES, (t + 1) * LANES)
                    into[:, cut] = into[:, cut] + half_rden[r, :, cut] * term

        drain(rows_in.at[it, :, pl.ds(0, SUB * width), :], row_recv.at[it])
        for t in range(tiles):
            e = [rows_in[it, t, pl.ds(k, SUB, stride=4), :] for k in range(1, 4)]
            half = (e[0] - e[1]) * 0.5
            tau = jnp.sqrt(half * half + e[2] * e[2] + 0.25)
            over = jnp.maximum((tau + 0.35 * (e[0] + e[1])) * fixed_rows[t], 1.0)
            HQ[t] = factor * (1.0 - 1.0 / over)
        halos = [[None] * tiles for _ in range(width)]
        head = (sub == 0) | (sub == 4)
        for m in range(width):
            for t in range(tiles):
                fq = jnp.where(sub < 4, HQ[t, 2 * m : 2 * m + 1, :], HQ[t, 2 * m + 1 : 2 * m + 2, :])
                raw = rows_in[it, t, SUB * m : SUB * (m + 1), :]
                halos[m][t] = raw * (1.0 - fq) + jnp.where(head, fq, 0.0)
        for r, total in row_terms(halos):
            C[r] = total * rden_rows[r]
        for f in range(4):
            for r in range(R):
                into = Z.at[0, r] if f == 0 else state.at[f - 1, r]
                for t in range(tiles):
                    cut = slice(t * LANES, (t + 1) * LANES)
                    into[:, cut] = into[:, cut] + row_term(r, f, t)

        drain(stat_in.at[it, pl.ds(1, n - 1)], stat_send)
        drain(rows_out.at[it], row_send)
        drain(lat_in.at[it], slab_send)

        @pl.when(is_last)
        def _():
            drain(fold_in.at[it, pl.ds(0, nlon - 1)], slab_send)

        return carry

    lax.fori_loop(0, ITERS, iteration, 0)
    outputs = (damage_ref, stress_ref.at[0], stress_ref.at[1], stress_ref.at[2])
    for t in range(tiles):
        cut = slice(t * LANES, t * LANES + span[t])
        for k, target in enumerate(outputs):
            for r in range(R):
                value = Z[0, r, :, t * LANES : (t + 1) * LANES] if k == 0 else state[k - 1, r, :, t * LANES : (t + 1) * LANES]
                stage[k, t, pl.ds(r, SUB, stride=R), :] = value
            target[:, cut] = stage[k, t, :, : span[t]]


def write_out(stress_vmem, damage_vmem, mean_vmem, stress_hbm, damage_hbm, mean_hbm, mean_smem, sem):
    copies = [
        pltpu.make_async_copy(stress_vmem, stress_hbm, sem.at[0]),
        pltpu.make_async_copy(damage_vmem, damage_hbm, sem.at[1]),
        pltpu.make_async_copy(mean_smem, mean_hbm, sem.at[2]),
    ]
    copies[0].start()
    copies[1].start()
    row = mean_vmem[0:1, :]
    for k in range(ITERS):
        mean_smem[k] = row[0, k]
    copies[2].start()
    for copy in copies:
        copy.wait()


def shards(nlon, nlat, strain_rate, stress_start, concentration, cell_class, land_mask, fold_partner, kernel_weights):
    ncols, nrows = concentration.shape
    side = kernel_weights.shape[0]
    width = side // 2
    R = ncols // SUB
    L = -(-(nrows + 2 * width) // LANES) * LANES
    tiles = L // LANES
    n = nlon * nlat
    V = lambda *shape: pltpu.VMEM(shape, F32)
    B = lambda *shape: pltpu.VMEM(shape, jnp.bfloat16)
    S = lambda *shape: pltpu.SemaphoreType.DMA(shape)
    planes = R + 2 * width
    ext = -(-(ncols + 2 * width) // SUB) * SUB
    hbm = pl.BlockSpec(memory_space=pltpu.HBM)
    vmem = pl.BlockSpec(memory_space=pltpu.VMEM)
    stress, damage, mean = pl.pallas_call(
        functools.partial(kernel, nlon, nlat, nrows, R, L, side),
        out_shape=(
            pltpu.VMEM((3, ncols, nrows), F32),
            pltpu.VMEM((ncols, nrows), F32),
            pltpu.VMEM((SUB, LANES), F32),
        ),
        in_specs=[hbm] * 7,
        out_specs=(vmem,) * 3,
        scratch_shapes=[
            pltpu.SMEM(kernel_weights.shape, F32), pltpu.SMEM(fold_partner.shape, jnp.int32),
            pltpu.SMEM((ncols + 2 * width,), jnp.int32),
            V(10, R, SUB, L), V(10, R, SUB, L), B(planes * tiles * SUB, 256), B(planes * tiles * SUB, 256),
            B((side + 1) * LANES, 256), B((side + 1) * LANES, 256),
            V(3, R, SUB, L), V(R, SUB, L), V(R, SUB, L), V(R, SUB, L), V(R, SUB, L), V(R, SUB, L), V(3, R, SUB, L),
            V(ITERS, tiles, SUB * width, LANES), V(ITERS, tiles, SUB * (width + 1), LANES),
            V(2, 2, 4, L), V(2, 2, 4, L), V(tiles, SUB, LANES), V(tiles, SUB, LANES),
            V(width * side, SUB, LANES), V(width * side, SUB, LANES), V(width, SUB, L), V(width, SUB, L),
            V(ITERS, 2, SUB, LANES), V(ITERS, 3, SUB, LANES), V(ITERS, nlon, SUB, LANES),
            V(nlon * R * SUB, LANES), V(ext, LANES), V(2, R, SUB, LANES),
            V(ITERS, 2, LANES), V(ITERS, n, 2, LANES), V(9, tiles, ncols, LANES),
            V(3, ncols, nrows), V(3, ncols, nrows), V(ncols, nrows),
            pltpu.VMEM((ncols, nrows), jnp.int32), pltpu.VMEM((ncols, nrows), jnp.int32),
            S(7), pltpu.SemaphoreType.DMA, pltpu.SemaphoreType.DMA, pltpu.SemaphoreType.DMA, S(ITERS),
            pltpu.SemaphoreType.DMA, S(ITERS), S(ITERS), pltpu.SemaphoreType.DMA, S(ITERS),
        ],
        compiler_params=pltpu.CompilerParams(
            collective_id=0, has_side_effects=True, vmem_limit_bytes=67043328 - 1024 * 1024
        ),
    )(kernel_weights, fold_partner, strain_rate, stress_start, concentration, cell_class, land_mask)
    return pl.pallas_call(
        write_out,
        out_shape=(
            jax.ShapeDtypeStruct((3, ncols, nrows), F32),
            jax.ShapeDtypeStruct((ncols, nrows), F32),
            jax.ShapeDtypeStruct((ITERS,), F32),
        ),
        in_specs=[vmem] * 3,
        out_specs=(hbm,) * 3,
        scratch_shapes=[pltpu.SMEM((ITERS,), F32), S(3)],
    )(*(pltpu.with_memory_space_constraint(x, pltpu.VMEM) for x in (stress, damage, mean)))


def solution(mesh):
    in_specs = (
        P(None, "lon", "lat"),
        P(None, "lon", "lat"),
        P("lon", "lat"),
        P(("member", "lon"), "lat"),
        P("lon", "lat"),
        P(),
        P(),
    )
    out_specs = (P(None, ("member", "lon"), "lat"), P(("member", "lon"), "lat"), P("member"))
    body = functools.partial(shards, mesh.shape["lon"], mesh.shape["lat"])
    return jax.shard_map(body, mesh=mesh, in_specs=in_specs, out_specs=out_specs, check_vma=False)
```

```python
import functools

import jax
import jax.numpy as jnp
from jax import lax
from jax.experimental import pallas as pl
from jax.experimental.pallas import tpu as pltpu
from jax.sharding import PartitionSpec as P

ITERS = 3
LANES = 128
SUB = 8
NORTH = 66
MESH = pl.DeviceIdType.MESH
F32 = jnp.float32


def kernel(
    nlon, nlat, nrows, R, L, side,
    w_hbm, partner_hbm, e_hbm, s_hbm, conc_hbm, class_hbm, mask_hbm,
    stress_ref, damage_ref, mean_ref,
    w_ref, partner_ref, where_ref,
    Z, Y, XH, XL, TH, TL, load, base, ocean, orl, half_ocean, half_rden, state,
    rows_out, rows_in, fixed_out, fixed_in, fixed_rows, HQ, WR, WC, C, rden_rows,
    slab, lat_in, fold_in, tops, D, T, stat, stat_in, stage,
    e_ref, s_ref, conc_ref, class_ref, mask_ref,
    in_sem, fixed_send, fixed_recv, row_send, row_recv, slab_send, lat_recv, fold_recv, stat_send, stat_recv,
):
    width = side // 2
    n = nlon * nlat
    ncols = R * SUB
    tiles = L // LANES
    lon, lat = lax.axis_index("lon"), lax.axis_index("lat")
    member = lax.axis_index("member")
    is_last = lat == nlat - 1
    me = lon * nlat + lat
    nb = nrows - (L - LANES)

    def dev(a, b):
        return (member, a, b)

    def peer(d):
        other = lax.rem(me + d, n)
        return dev(other // nlat, lax.rem(other, nlat))

    def every(first, last, body):
        if last - first <= 16:
            for d in range(first, last):
                body(d)
        else:
            lax.fori_loop(first, last, lambda d, c: (body(d), c)[1], 0)

    def tile(x, t):
        return x[:, t * LANES : (t + 1) * LANES]

    right, left = lax.rem(lon + 1, nlon), lax.rem(lon + nlon - 1, nlon)
    other_lat = lax.rem(lat + 1, nlat)

    loads = [
        pltpu.make_async_copy(a, b, in_sem.at[k])
        for k, (a, b) in enumerate((
            (mask_hbm, mask_ref), (conc_hbm, conc_ref), (class_hbm, class_ref), (s_hbm, s_ref), (e_hbm, e_ref),
            (w_hbm, w_ref), (partner_hbm, partner_ref),
        ))
    ]
    for copy in loads:
        copy.start()
    barrier = pltpu.get_barrier_semaphore()
    every(1, n, lambda d: pl.semaphore_signal(barrier, inc=1, device_id=peer(d), device_id_type=MESH))

    sub = lax.broadcasted_iota(jnp.int32, (SUB, LANES), 0)
    sub_wide = lax.broadcasted_iota(jnp.int32, (SUB, L), 0)
    lane = lax.broadcasted_iota(jnp.int32, (SUB, LANES), 1)
    slot = lax.rem(lane, width)
    packed_slot = lax.rem(lax.rem(lane, 16), width)

    edge = jnp.zeros((SUB, LANES), F32)
    for r in range(R):
        for ref in (base.at[r], ocean.at[r], orl.at[r], *(load.at[k, r] for k in range(3)), Z.at[0, r],
                    *(state.at[k, r] for k in range(3))):
            ref[:, L - LANES :] = edge
    for t in range(tiles):
        for it in range(ITERS):
            rows_in[it, t, SUB * width :, :] = edge
        fixed_rows[t] = edge
    mean_ref[...] = edge
    span = [min(LANES, nrows - t * LANES) for t in range(tiles)]

    def regroup(first, refs, t):
        cut = slice(t * LANES, t * LANES + span[t])
        for k, source in enumerate(refs):
            stage[first + k, t, :, : span[t]] = source[:, cut].astype(F32)
        for r in range(R):
            yield r, cut, [
                stage[first + k, t, pl.ds(r, SUB, stride=R), :][:, : span[t]] for k in range(len(refs))
            ]

    for copy in loads[:2]:
        copy.wait()
    count = jnp.zeros((SUB, LANES), F32)
    for t in range(tiles):
        for r, cut, (oc, conc) in regroup(0, (mask_ref, conc_ref), t):
            ocean[r, :, cut] = oc
            orl[r, :, cut] = oc / (0.6 * conc)
            base[r, :, cut] = conc * jnp.exp(-2.0 * (1.0 - conc))
            Z[0, r, :, cut] = oc * 0.1 * conc
    for m in range(width):
        fixed_out[0, 0, m : m + 1, :] = orl[R - width + m, SUB - 1 : SUB, :]
        fixed_out[0, 1, m : m + 1, :] = ocean[R - width + m, SUB - 1 : SUB, :]
        fixed_out[1, 0, m : m + 1, :] = orl[width - 1 - m, 0:1, :]
        fixed_out[1, 1, m : m + 1, :] = ocean[width - 1 - m, 0:1, :]

    def fixed_copy(k, to):
        return pltpu.make_async_remote_copy(
            src_ref=fixed_out.at[k, :, pl.ds(0, width), :], dst_ref=fixed_in.at[k, :, pl.ds(0, width), :],
            send_sem=fixed_send, recv_sem=fixed_recv, device_id=dev(to, lat), device_id_type=MESH,
        )

    def far_first(up, down):
        odd = lax.rem(lon, 2) == 1

        @pl.when(odd)
        def _():
            up()
            down()

        @pl.when(jnp.logical_not(odd))
        def _():
            down()
            up()

    for copy in loads[2:4]:
        copy.wait()
    for t in range(tiles):
        for r, cut, (grade, s1, s2, s3) in regroup(2, (class_ref, s_ref.at[0], s_ref.at[1], s_ref.at[2]), t):
            oc = ocean[r, :, cut]
            Z[0, r, :, cut] = Z[0, r, :, cut] * grade
            for k, part in enumerate((s1, s2, s3)):
                state[k, r, :, cut] = oc * part
    for r in range(R):
        oc = ocean[r]
        Z[8, r] = oc
        Z[9, r] = jnp.zeros((SUB, L), F32)
        half_ocean[r] = 0.5 * oc
        for t in range(tiles):
            count = count + tile(oc, t)
    loads[4].wait()
    for t in range(tiles):
        for r, cut, (one, two, shear) in regroup(6, (e_ref.at[0], e_ref.at[1], e_ref.at[2]), t):
            load[0, r, :, cut] = (one + two / 3.0) / (8.0 / 9.0)
            load[1, r, :, cut] = (two + one / 3.0) / (8.0 / 9.0)
            load[2, r, :, cut] = (shear / (4.0 / 3.0)) / (8.0 / 9.0)
    count = jnp.sum(count, axis=0, keepdims=True)
    pl.semaphore_wait(barrier, n - 1)
    far_first(lambda: fixed_copy(0, right).start(), lambda: fixed_copy(1, left).start())

    def build_tables():
        for copy in loads[5:]:
            copy.wait()
        for d in range(width):
            for b in range(side):
                WR[d * side + b] = jnp.where(sub < 4, w_ref[d, b], w_ref[side - 1 - d, b])
        span_lanes = 5 * width
        for d in range(1, width + 1):
            keep = (slot >= width - d) & ((lane < span_lanes) | ((lane >= NORTH) & (lane < NORTH + span_lanes)))
            for a in range(side):
                WC[(d - 1) * side + a] = jnp.where(
                    keep, jnp.where(lane < NORTH - width, w_ref[a, width - d], w_ref[a, width + d]), 0.0
                )
        for i in range(ncols + 2 * width):
            p = partner_ref[lax.rem(lon * ncols + i - width + nlon * ncols, nlon * ncols)]
            col = lax.rem(p, ncols)
            where_ref[i] = ((p // ncols) * R + lax.rem(col, R)) * SUB + col // R

    pairs = (R + 2 * width) // 2
    taps = (side + 1) // 2
    step = LANES - 2 * width
    block = 2 * tiles * SUB

    def build_bands():
        for strip in range(LANES // 16):
            row = lax.broadcasted_iota(jnp.int32, (16, LANES), 0)
            offset = row + 16 * strip + width - lax.broadcasted_iota(jnp.int32, (16, LANES), 1)
            hits = [offset == b for b in range(side)]
            for a in range(-1, side + 1):
                band = jnp.zeros((16, LANES), F32)
                if 0 <= a < side:
                    for b in range(side):
                        band = jnp.where(hits[b], w_ref[a, b], band)
                high = band.astype(jnp.bfloat16)
                low = (band - high.astype(F32)).astype(jnp.bfloat16)
                for k in range(taps):
                    for u in range(2):
                        for v in range(2):
                            if 2 * k + u - v == a:
                                at = (slice(k * 256 + u * LANES + 16 * strip, k * 256 + u * LANES + 16 * strip + 16),
                                      slice(v * LANES, (v + 1) * LANES))
                                TH[at] = high
                                TL[at] = low

    def build(g, buf):
        chunks = []
        for r in range(R):
            plane = []
            for i in range(2):
                last = None
                for t in range(tiles):
                    shift = width + (LANES - step) * t
                    here = Z[2 * g + i, r, :, t * LANES : (t + 1) * LANES]
                    now = pltpu.roll(here, shift, 1)
                    before = 0.0 if last is None else pltpu.roll(last, shift, 1)
                    plane.append(jnp.where(lane < shift, before, now))
                    last = here
            chunks.append(plane)
        for p in range(R + 2 * width):
            if p < width:
                plane = [jnp.where(sub == 0, 0.0, pltpu.roll(x, 1, 0)) for x in chunks[p + R - width]]
            elif p < width + R:
                plane = chunks[p - width]
            else:
                plane = [jnp.where(sub == SUB - 1, 0.0, pltpu.roll(x, SUB - 1, 0)) for x in chunks[p - width - R]]
            for j in range(tiles):
                x = jnp.concatenate(plane[2 * j : 2 * j + 2], axis=0)
                high = x.astype(jnp.bfloat16)
                at = (slice((p // 2) * block + 16 * j, (p // 2) * block + 16 * j + 16),
                      slice((p % 2) * LANES, (p % 2 + 1) * LANES))
                XH[(buf, *at)] = high
                XL[(buf, *at)] = (x - high.astype(F32)).astype(jnp.bfloat16)

    def multiply(g, buf):
        out = None
        for k in range(taps):
            rows = slice(k * block, k * block + (R // 2) * block)
            band = slice(k * 256, (k + 1) * 256)
            for x, w in ((XH, TH), (XL, TH), (XH, TL)):
                term = jnp.dot(x[buf, rows, :], w[band, :], preferred_element_type=F32)
                out = term if out is None else out + term
        for r in range(R):
            for i in range(2):
                def part(t):
                    row = (r // 2) * block + (i * tiles + t) * SUB
                    return out[row : row + SUB, (r % 2) * LANES : (r % 2 + 1) * LANES]
                for t in range(tiles):
                    first = width + (LANES - step) * t
                    value = pltpu.roll(part(t), LANES - first, 1)
                    if t + 1 < tiles:
                        rest = pltpu.roll(part(t + 1), LANES - width - first - width, 1)
                        value = jnp.where(lane < LANES - width - first, value, rest)
                    Y[2 * g + i, r, :, t * LANES : (t + 1) * LANES] = value

    def row_terms(halos):
        for r in range(width):
            total = None
            for b in range(side):
                parts = []
                for t in range(tiles):
                    acc = None
                    for m in range(r, width):
                        term = WR[(m - r) * side + b] * halos[m][t]
                        acc = term if acc is None else acc + term
                    parts.append(acc)
                wide = jnp.concatenate(parts, axis=1)
                wide = wide if b == width else pltpu.roll(wide, (width - b) % L, 1)
                total = wide if total is None else total + wide
            yield r, total

    def row_term(p, f, t):
        cut = slice(t * LANES, (t + 1) * LANES)
        out = jnp.zeros((SUB, LANES), F32)
        if p < width:
            out = jnp.where(sub == 0, C[p, f : f + 1, cut], out)
        if R - 1 - p < width:
            out = jnp.where(sub == SUB - 1, C[R - 1 - p, 4 + f : 5 + f, cut], out)
        return out

    def flip(x, at):
        y = jnp.where(at == 0, pltpu.roll(x, LANES - (width - 1), 1), x)
        return jnp.where(at == width - 1, pltpu.roll(x, width - 1, 1), y)

    def column_term(f, p):
        at = width * f + width
        south = jnp.where(lane < width, pltpu.roll(T[0, p], (LANES - at) % LANES, 1), 0.0)
        north = jnp.where(
            (lane >= nb - width) & (lane < nb), pltpu.roll(T[1, p], (nb - width - NORTH - at) % LANES, 1), 0.0
        )
        return south, north

    def iteration(it, carry):
        excess = jnp.zeros((SUB, LANES), F32)
        for r in range(R):
            oc = ocean[r]
            damage = Z[0, r]
            keep = 1.0 - damage
            square = keep * keep
            scale = oc * square / (square + 0.5)
            bk = base[r] * keep
            el = [scale * (state[k, r] + bk * load[k, r]) for k in range(3)]
            half = (el[0] - el[1]) * 0.5
            tau = half * half + el[2] * el[2] + 0.25
            tau = tau * lax.rsqrt(tau)
            over = jnp.maximum((tau + 0.35 * (el[0] + el[1])) * orl[r], 1.0)
            q = 1.0 - 1.0 / over
            for t in range(tiles):
                excess = excess + (tile(over, t) - 1.0)
            Z[4, r] = keep * q
            for k in range(3):
                Z[1 + k, r] = el[k]
                Z[5 + k, r] = el[k] * q
            for m in range(width):
                for f, part in enumerate((damage, *el)):
                    for t in range(tiles):
                        if r == R - width + m:
                            rows_out[it, t, SUB * m + f : SUB * m + f + 1, :] = tile(part, t)[SUB - 1 : SUB]
                        if r == width - 1 - m:
                            rows_out[it, t, SUB * m + 4 + f : SUB * m + 5 + f, :] = tile(part, t)[0:1]
        stat[it, 0:1, :] = jnp.sum(excess, axis=0, keepdims=True)
        stat[it, 1:2, :] = count

        def stat_copy(d):
            return pltpu.make_async_remote_copy(
                src_ref=stat.at[it], dst_ref=stat_in.at[it, d], send_sem=stat_send,
                recv_sem=stat_recv.at[it], device_id=peer(d), device_id_type=MESH,
            )

        def row_copy(s, m, to):
            piece = pl.ds(SUB * m + 4 * s, 4)
            return pltpu.make_async_remote_copy(
                src_ref=rows_out.at[it, :, piece, :], dst_ref=rows_in.at[it, :, piece, :], send_sem=row_send,
                recv_sem=row_recv.at[it], device_id=dev(to, lat), device_id_type=MESH,
            )

        def start_rows(s, to, ms):
            for m in ms:
                row_copy(s, m, to).start()

        every(1, n, lambda d: stat_copy(d).start())
        far_first(lambda: start_rows(0, right, [0]), lambda: start_rows(1, left, [0]))

        low = jnp.zeros((SUB, LANES), F32)
        high = jnp.zeros((SUB, LANES), F32)
        for r in range(R):
            for f in range(9):
                at = 32 * r + (width * f if f < 4 else (16 + width * (f - 4) if f < 8 else 4 * width))
                here = (lane >= at) & (lane < at + width)
                low = jnp.where(here, pltpu.roll(Z[f, r, :, :LANES], at, 1), low)
                high = jnp.where(here, pltpu.roll(Z[f, r, :, L - LANES :], (at + width - nb) % LANES, 1), high)
        slab[it, 0] = jnp.where(is_last, low, high)
        slab[it, 1] = high

        def lat_copy(k):
            to = lax.rem(lon + 1 - k + nlon, nlon)
            return pltpu.make_async_remote_copy(
                src_ref=slab.at[it, 0], dst_ref=lat_in.at[it, k], send_sem=slab_send,
                recv_sem=lat_recv.at[it], device_id=dev(to, other_lat), device_id_type=MESH,
            )

        def fold_copy(d):
            return pltpu.make_async_remote_copy(
                src_ref=slab.at[it, 1], dst_ref=fold_in.at[it, lon],
                send_sem=slab_send, recv_sem=fold_recv.at[it],
                device_id=dev(lax.rem(lon + d, nlon), lat), device_id_type=MESH,
            )

        @pl.when(is_last)
        def _():
            every(1, nlon, lambda d: fold_copy(d).start())
            fold_in[it, lon] = slab[it, 1]

        for k in range(3):
            lat_copy(k).start()

        rest = list(range(1, width))
        far_first(lambda: start_rows(0, right, rest), lambda: start_rows(1, left, rest))

        @pl.when(it == 0)
        def _():
            build_tables()
            build_bands()
            build(4, 1)
            multiply(4, 1)

        build(0, 0)
        for g in range(4):
            if g + 1 < 4:
                build(g + 1, (g + 1) % 2)
            multiply(g, g % 2)

        def drain(ref, sem):
            pltpu.make_async_copy(ref, ref, sem).wait()

        def wait_slabs():
            drain(lat_in.at[it], lat_recv.at[it])

            @pl.when(is_last)
            def _():
                drain(fold_in.at[it, pl.ds(0, nlon - 1)], fold_recv.at[it])

        def fold_in_place():
            for r in range(R):
                for t in range(tiles):
                    cut = slice(t * LANES, (t + 1) * LANES)
                    ho, hr = half_ocean[r, :, cut], half_rden[r, :, cut]
                    for f in range(8):
                        Y[f, r, :, cut] = ho * Z[f, r, :, cut] + hr * Y[f, r, :, cut]

        @pl.when(it > 0)
        def _():
            fold_in_place()

        drain(stat_in.at[it, pl.ds(1, n - 1)], stat_recv.at[it])
        total = stat[it]
        if n <= 16:
            for d in range(1, n):
                total = total + stat_in[it, d]
        else:
            total = lax.fori_loop(1, n, lambda d, c: c + stat_in[it, d], total)
        sums = jnp.sum(total, axis=1, keepdims=True)
        mean = sums[0:1] / (sums[1:2] + 1.0)
        factor = 1.0 / (1.0 + 2.0 * mean)
        mean_ref[...] = jnp.where(lane == it, mean, mean_ref[...])

        def columns():
            signed = jnp.where(lax.rem(lane, 32) < width, factor, -factor)

            @pl.when(is_last)
            def _():
                def spread(k):
                    got = fold_in[it, k]
                    got = got + signed * pltpu.roll(got, LANES - 16, 1)
                    for r in range(R):
                        tops[pl.ds((k * R + r) * SUB, SUB), :] = pltpu.roll(got, (NORTH - 32 * r) % LANES, 1)

                every(0, nlon, spread)
                for i in range(ncols + 2 * width):
                    D[i : i + 1, :] = tops[pl.ds(where_ref[i], 1), :]

            south_side = lane < NORTH - width
            own = []
            for k in range(3):
                got = lat_in[it, k]
                got = got + signed * pltpu.roll(got, LANES - 16, 1)
                own.append(jnp.where(is_last, got, flip(got, packed_slot)))

            def piece(k, r):
                return jnp.where(
                    is_last, pltpu.roll(own[k], (LANES - 32 * r) % LANES, 1),
                    pltpu.roll(own[k], (NORTH - 32 * r) % LANES, 1),
                )

            mid = [piece(1, r) for r in range(R)]
            ghosts = [None] * (R + 2 * width)
            for r in range(R):
                ghosts[width + r] = mid[r]
            for m in range(width):
                r = m + R - width
                ghosts[m] = jnp.where(sub == 0, pltpu.roll(piece(0, r), 1, 0), pltpu.roll(mid[r], 1, 0))
                ghosts[R + width + m] = jnp.where(
                    sub == SUB - 1, pltpu.roll(piece(2, m), SUB - 1, 0), pltpu.roll(mid[m], SUB - 1, 0)
                )
            for p in range(R + 2 * width):
                fold = D[pl.ds(p, SUB, stride=R), :]
                ghosts[p] = jnp.where(
                    south_side, jnp.where(is_last, ghosts[p], 0.0), jnp.where(is_last, fold, ghosts[p])
                )
            for r in range(R):
                total = None
                for d in range(1, width + 1):
                    acc = None
                    for a in range(side):
                        term = WC[(d - 1) * side + a] * ghosts[r + a]
                        acc = term if acc is None else acc + term
                    acc = pltpu.roll(acc, d, 1)
                    total = acc if total is None else total + acc
                T[0, r] = total
                T[1, r] = flip(total, slot)

        def finish_ocean():
            drain(fixed_in.at[:, :, pl.ds(0, width), :], fixed_recv)
            drain(fixed_in.at[:, :, pl.ds(0, width), :], fixed_send)
            for t in range(tiles):
                cut = slice(t * LANES, (t + 1) * LANES)
                for m in range(width):
                    for s in range(2):
                        fixed_rows[t, 2 * m + s : 2 * m + s + 1, :] = fixed_in[s, 0, m : m + 1, cut]
            halos = [
                [
                    jnp.where(
                        sub < 4, fixed_in[0, 1, m : m + 1, t * LANES : (t + 1) * LANES],
                        fixed_in[1, 1, m : m + 1, t * LANES : (t + 1) * LANES],
                    )
                    for t in range(tiles)
                ]
                for m in range(width)
            ]
            for r, total in row_terms(halos):
                C[r] = total
            for r in range(R):
                south, north = column_term(4, r)
                for t in range(tiles):
                    cut = slice(t * LANES, (t + 1) * LANES)
                    denom = Y[8, r, :, cut] + row_term(r, 0, t)
                    if t == 0:
                        denom = denom + south
                    if t == tiles - 1:
                        denom = denom + north
                    half_rden[r, :, cut] = half_ocean[r, :, cut] / (denom + 1.0)
            for r in range(width):
                rden_rows[r] = jnp.where(
                    sub_wide < 4, half_rden[r, 0:1, :], half_rden[R - 1 - r, SUB - 1 : SUB, :]
                )

        @pl.when(it == 0)
        def _():
            wait_slabs()
            columns()
            finish_ocean()
            fold_in_place()

        for r in range(R):
            for t in range(tiles):
                cut = slice(t * LANES, (t + 1) * LANES)
                for f in range(4):
                    part = factor if f == 0 else -factor
                    fresh = Y[f, r, :, cut] + part * Y[4 + f, r, :, cut]
                    if f == 0:
                        Z[0, r, :, cut] = fresh
                    else:
                        state[f - 1, r, :, cut] = fresh

        @pl.when(it > 0)
        def _():
            wait_slabs()
            columns()

        for f in range(4):
            for r in range(R):
                into = Z.at[0, r] if f == 0 else state.at[f - 1, r]
                south, north = column_term(f, r)
                for t, term in ((0, south), (tiles - 1, north)):
                    cut = slice(t * LANES, (t + 1) * LANES)
                    into[:, cut] = into[:, cut] + half_rden[r, :, cut] * term

        drain(rows_in.at[it, :, pl.ds(0, SUB * width), :], row_recv.at[it])
        for t in range(tiles):
            e = [rows_in[it, t, pl.ds(k, SUB, stride=4), :] for k in range(1, 4)]
            half = (e[0] - e[1]) * 0.5
            tau = half * half + e[2] * e[2] + 0.25
            tau = tau * lax.rsqrt(tau)
            over = jnp.maximum((tau + 0.35 * (e[0] + e[1])) * fixed_rows[t], 1.0)
            HQ[t] = factor * (1.0 - 1.0 / over)
        halos = [[None] * tiles for _ in range(width)]
        head = (sub == 0) | (sub == 4)
        for m in range(width):
            for t in range(tiles):
                fq = jnp.where(sub < 4, HQ[t, 2 * m : 2 * m + 1, :], HQ[t, 2 * m + 1 : 2 * m + 2, :])
                raw = rows_in[it, t, SUB * m : SUB * (m + 1), :]
                halos[m][t] = raw * (1.0 - fq) + jnp.where(head, fq, 0.0)
        for r, total in row_terms(halos):
            C[r] = total * rden_rows[r]
        for f in range(4):
            for r in range(R):
                into = Z.at[0, r] if f == 0 else state.at[f - 1, r]
                for t in range(tiles):
                    cut = slice(t * LANES, (t + 1) * LANES)
                    into[:, cut] = into[:, cut] + row_term(r, f, t)

        drain(stat_in.at[it, pl.ds(1, n - 1)], stat_send)
        drain(rows_out.at[it], row_send)
        drain(lat_in.at[it], slab_send)

        @pl.when(is_last)
        def _():
            drain(fold_in.at[it, pl.ds(0, nlon - 1)], slab_send)

        return carry

    lax.fori_loop(0, ITERS, iteration, 0)
    outputs = (damage_ref, stress_ref.at[0], stress_ref.at[1], stress_ref.at[2])
    for t in range(tiles):
        cut = slice(t * LANES, t * LANES + span[t])
        for k, target in enumerate(outputs):
            for r in range(R):
                value = Z[0, r, :, t * LANES : (t + 1) * LANES] if k == 0 else state[k - 1, r, :, t * LANES : (t + 1) * LANES]
                stage[k, t, pl.ds(r, SUB, stride=R), :] = value
            target[:, cut] = stage[k, t, :, : span[t]]


def write_out(stress_vmem, damage_vmem, mean_vmem, stress_hbm, damage_hbm, mean_hbm, mean_smem, sem):
    copies = [
        pltpu.make_async_copy(stress_vmem, stress_hbm, sem.at[0]),
        pltpu.make_async_copy(damage_vmem, damage_hbm, sem.at[1]),
        pltpu.make_async_copy(mean_smem, mean_hbm, sem.at[2]),
    ]
    copies[0].start()
    copies[1].start()
    row = mean_vmem[0:1, :]
    for k in range(ITERS):
        mean_smem[k] = row[0, k]
    copies[2].start()
    for copy in copies:
        copy.wait()


def shards(nlon, nlat, strain_rate, stress_start, concentration, cell_class, land_mask, fold_partner, kernel_weights):
    ncols, nrows = concentration.shape
    side = kernel_weights.shape[0]
    width = side // 2
    R = ncols // SUB
    L = -(-(nrows + 2 * width) // LANES) * LANES
    tiles = L // LANES
    n = nlon * nlat
    V = lambda *shape: pltpu.VMEM(shape, F32)
    B = lambda *shape: pltpu.VMEM(shape, jnp.bfloat16)
    S = lambda *shape: pltpu.SemaphoreType.DMA(shape)
    planes = R + 2 * width
    ext = -(-(ncols + 2 * width) // SUB) * SUB
    hbm = pl.BlockSpec(memory_space=pltpu.HBM)
    vmem = pl.BlockSpec(memory_space=pltpu.VMEM)
    stress, damage, mean = pl.pallas_call(
        functools.partial(kernel, nlon, nlat, nrows, R, L, side),
        out_shape=(
            pltpu.VMEM((3, ncols, nrows), F32),
            pltpu.VMEM((ncols, nrows), F32),
            pltpu.VMEM((SUB, LANES), F32),
        ),
        in_specs=[hbm] * 7,
        out_specs=(vmem,) * 3,
        scratch_shapes=[
            pltpu.SMEM(kernel_weights.shape, F32), pltpu.SMEM(fold_partner.shape, jnp.int32),
            pltpu.SMEM((ncols + 2 * width,), jnp.int32),
            V(10, R, SUB, L), V(10, R, SUB, L), B(2, planes * tiles * SUB, 256), B(2, planes * tiles * SUB, 256),
            B((side + 1) * LANES, 256), B((side + 1) * LANES, 256),
            V(3, R, SUB, L), V(R, SUB, L), V(R, SUB, L), V(R, SUB, L), V(R, SUB, L), V(R, SUB, L), V(3, R, SUB, L),
            V(ITERS, tiles, SUB * width, LANES), V(ITERS, tiles, SUB * (width + 1), LANES),
            V(2, 2, 4, L), V(2, 2, 4, L), V(tiles, SUB, LANES), V(tiles, SUB, LANES),
            V(width * side, SUB, LANES), V(width * side, SUB, LANES), V(width, SUB, L), V(width, SUB, L),
            V(ITERS, 2, SUB, LANES), V(ITERS, 3, SUB, LANES), V(ITERS, nlon, SUB, LANES),
            V(nlon * R * SUB, LANES), V(ext, LANES), V(2, R, SUB, LANES),
            V(ITERS, 2, LANES), V(ITERS, n, 2, LANES), V(9, tiles, ncols, LANES),
            V(3, ncols, nrows), V(3, ncols, nrows), V(ncols, nrows),
            pltpu.VMEM((ncols, nrows), jnp.int32), pltpu.VMEM((ncols, nrows), jnp.int32),
            S(7), pltpu.SemaphoreType.DMA, pltpu.SemaphoreType.DMA, pltpu.SemaphoreType.DMA, S(ITERS),
            pltpu.SemaphoreType.DMA, S(ITERS), S(ITERS), pltpu.SemaphoreType.DMA, S(ITERS),
        ],
        compiler_params=pltpu.CompilerParams(
            collective_id=0, has_side_effects=True, vmem_limit_bytes=67043328 - 1024 * 1024
        ),
    )(kernel_weights, fold_partner, strain_rate, stress_start, concentration, cell_class, land_mask)
    return pl.pallas_call(
        write_out,
        out_shape=(
            jax.ShapeDtypeStruct((3, ncols, nrows), F32),
            jax.ShapeDtypeStruct((ncols, nrows), F32),
            jax.ShapeDtypeStruct((ITERS,), F32),
        ),
        in_specs=[vmem] * 3,
        out_specs=(hbm,) * 3,
        scratch_shapes=[pltpu.SMEM((ITERS,), F32), S(3)],
    )(*(pltpu.with_memory_space_constraint(x, pltpu.VMEM) for x in (stress, damage, mean)))


def solution(mesh):
    in_specs = (
        P(None, "lon", "lat"),
        P(None, "lon", "lat"),
        P("lon", "lat"),
        P(("member", "lon"), "lat"),
        P("lon", "lat"),
        P(),
        P(),
    )
    out_specs = (P(None, ("member", "lon"), "lat"), P(("member", "lon"), "lat"), P("member"))
    body = functools.partial(shards, mesh.shape["lon"], mesh.shape["lat"])
    return jax.shard_map(body, mesh=mesh, in_specs=in_specs, out_specs=out_specs, check_vma=False)
```
